32 devices in a mesh: rep: 2 (over x), lev: 4 (over z), tile: 4 (over y, core).
Axes of the slice: x: 2, y: 2, z: 4, core: 2. Of those that a mesh axis runs over, the one named last changes fastest.
Arguments:
- tokens: bfloat16 [2, 8, 4, 8, 8, 768], P('rep', 'lev', 'tile'), may hold values from -6 to 6
- w_qkv: bfloat16 [768, 2304], P('tile'), may hold values from -0.21875 to 0.21875
- w_proj: bfloat16 [768, 768], P('tile'), may hold values from -0.21875 to 0.21875
- seam_codes: int32 [4, 2], replicated, may hold values from 0 to 1
- upstream: bfloat16 [2, 8, 4, 8, 8, 768], P('rep', 'lev', 'tile'), may hold values from -6 to 6
Outputs:
- output: bfloat16 [2, 8, 4, 8, 8, 768], P('rep', 'lev', 'tile')
- grad_tokens: bfloat16 [2, 8, 4, 8, 8, 768], P('rep', 'lev', 'tile')
- grad_qkv: float32 [768, 2304], P('tile')
- grad_proj: float32 [768, 768], P('tile')
The draws below stay inside these ranges and needn't reach their ends.
Inputs may be any that keep to these rules, and one draw needn't show every extreme that they name: The tiles form a periodic grid of four rows of 1 tiles: tile t's eastern neighbour is (t + 1) mod 4 and its northern neighbour (t + 1) mod 4. seam_codes[t, 0] is 1 where the seam to the eastern neighbour runs reversed, seam_codes[t, 1] likewise for the northern neighbour.
All inputs are finite; a program needn't handle non-finite values.
Results may differ from the reference program's by a relative error of at most 0.019.
Values may be sent and summed in bfloat16 or wider, within the bound.
No kernel may reach another device: no remote copies, remote signals or barrier semaphores. Data moves between devices by JAX's collectives and lax.ppermute only.
A program may use at most 64 MiB of HBM per device.

```python
import jax
import jax.numpy as jnp
from jax import lax

D = 768
HEAD_DIM = 32
WIN = 8
WIN_LEV = 2
S = 8
LEVELS = 8
TILES = 4
BATCH = 2


def plant(array, own_key, smallest, top_value):
    longest = array.shape.index(max(array.shape))
    spots = []
    for shift in (0, 1):
        where = [jax.random.randint(jax.random.fold_in(own_key, axis), (), 0, length) for axis, length in enumerate(array.shape)]
        where[longest] = (where[longest] + shift) % array.shape[longest]
        spots.append(tuple(where))
    return array.at[spots[0]].set(smallest).at[spots[1]].set(top_value)


def spiked(result, own_key, source, target, parts, factor):
    def block_of(axis_at):
        return (jnp.arange(result.shape[axis_at]) // (result.shape[axis_at] // parts)).reshape((-1,) + (1,) * (result.ndim - 1 - axis_at))

    near = jax.random.permutation(own_key, parts)[block_of(target)]
    far = (block_of(target) + parts // 2) % parts
    return jnp.where((block_of(source) == near) | (block_of(source) == far), factor * result, result)


def block_scale(key, shape, pieces, low, high):
    def one(position, shards_of):
        steps = jax.random.uniform(jax.random.fold_in(jax.random.fold_in(key, 6), position), (shards_of,), jnp.float32, low / len(pieces), high / len(pieces))
        return jnp.repeat(jnp.exp(steps), shape[position] // shards_of).reshape((-1,) + (1,) * (len(shape) - position - 1))

    gain = one(*pieces[0])
    for cut in pieces[1:]:
        gain = gain * one(*cut)
    return gain


def gaussian(stream_key, shape, width, most, shards=(), held_as=jnp.bfloat16):
    values = width * jax.random.normal(stream_key, shape, jnp.float32)
    if shards:
        values = values * block_scale(stream_key, shape, shards, -0.22, 0.18)
    return jnp.clip(values, -most, most).astype(held_as)


def heavy_noise(key, dims, deviation, bound, cuts, heavy, kind=jnp.bfloat16):
    drawn = deviation * jax.random.normal(key, dims, jnp.float32)
    if cuts:
        drawn = drawn * block_scale(key, dims, cuts, -0.22, 0.18)
    return jnp.clip(spiked(drawn, jax.random.fold_in(key, 3), *heavy), -bound, bound).astype(kind)


def setup_inputs(seed: int = 0) -> dict:
    seeds = jax.random.split(jax.random.key(seed), 6)
    return {
        "tokens": heavy_noise(seeds[0], (BATCH, LEVELS, TILES, S, S, D), 1.0, 6.0, ((0, 2), (1, 4), (2, 4)), (2, 5, 4, 2.0)),
        "w_qkv": gaussian(seeds[1], (D, 3 * D), D ** -0.5, 0.21875, ((0, 4),)),
        "w_proj": gaussian(seeds[2], (D, D), D ** -0.5, 0.21875, ((0, 4),)),
        "seam_codes": plant(jax.random.randint(seeds[3], (TILES, 2), 0, 2), jax.random.fold_in(seeds[3], 1), 0, 1).astype(jnp.int32),
        "upstream": heavy_noise(seeds[4], (BATCH, LEVELS, TILES, S, S, D), 1.0, 6.0, ((0, 2), (1, 4), (2, 4)), (2, 5, 4, 2.0)),
    }


EPSILON = 1e-05

def layer_stats(token_rows):
    values = token_rows.astype(jnp.float32)
    center = lax.optimization_barrier(jnp.mean(values, axis=1, keepdims=True))
    spread = lax.optimization_barrier(jnp.mean(jnp.square(values - center), axis=1, keepdims=True))
    inverse = lax.rsqrt(spread + EPSILON)
    return ((values - center) * inverse, inverse)

def norm_backward(upstream_rows, grad_hidden, normalized, inverse):
    centre = lax.optimization_barrier(jnp.mean(grad_hidden, axis=1, keepdims=True))
    projected = lax.optimization_barrier(jnp.mean(grad_hidden * normalized, axis=1, keepdims=True))
    total_grad = upstream_rows.astype(jnp.float32) + (grad_hidden - centre - normalized * projected) * inverse
    return total_grad.astype(jnp.bfloat16)

def roll_field(grid_field, seam_codes, north_step):
    shift_cells = WIN // 2
    east_flag = (seam_codes[:, 0] == 1)[None, None, :, None, None, None]
    north_flag = (seam_codes[:, 1] == 1)[None, None, :, None, None, None]
    east_part = jnp.roll(grid_field, -1, axis=2)[:, :, :, :, :shift_cells]
    east_part = jnp.where(east_flag, east_part[:, :, :, ::-1], east_part)
    across = jnp.concatenate([grid_field[:, :, :, :, shift_cells:], east_part], axis=4)
    north_part = jnp.roll(across, -north_step, axis=2)[:, :, :, :shift_cells]
    north_part = jnp.where(north_flag, north_part[:, :, :, :, ::-1], north_part)
    upward = jnp.concatenate([across[:, :, :, shift_cells:], north_part], axis=3)
    return jnp.roll(upward, -1, axis=1)

def unroll_field(rolled, seam_codes, north_step):
    shift_cells = WIN // 2
    extent = rolled.shape[3]
    east_flag = (seam_codes[:, 0] == 1)[None, None, :, None, None, None]
    north_flag = (seam_codes[:, 1] == 1)[None, None, :, None, None, None]
    upward = jnp.roll(rolled, 1, axis=1)
    north_part = upward[:, :, :, extent - shift_cells:]
    north_part = jnp.where(north_flag, north_part[:, :, :, :, ::-1], north_part)
    across = jnp.concatenate([jnp.roll(north_part, north_step, axis=2), upward[:, :, :, :extent - shift_cells]], axis=3)
    east_part = across[:, :, :, :, extent - shift_cells:]
    east_part = jnp.where(east_flag, east_part[:, :, :, ::-1], east_part)
    return jnp.concatenate([jnp.roll(east_part, 1, axis=2), across[:, :, :, :, :extent - shift_cells]], axis=4)

def to_windows(grid_field):
    levels = grid_field.shape[0]
    extent = grid_field.shape[1]
    channels = grid_field.shape[3]
    blocks = grid_field.reshape(levels // WIN_LEV, WIN_LEV, extent // WIN, WIN, extent // WIN, WIN, channels)
    blocks = blocks.transpose(0, 2, 4, 1, 3, 5, 6)
    return blocks.reshape(-1, WIN_LEV * WIN * WIN, channels)

def from_windows(windows, levels, extent):
    channels = windows.shape[-1]
    blocks = windows.reshape(levels // WIN_LEV, extent // WIN, extent // WIN, WIN_LEV, WIN, WIN, channels)
    blocks = blocks.transpose(0, 3, 1, 4, 2, 5, 6)
    return blocks.reshape(levels, extent, extent, channels)

def split_heads(packed):
    windows = packed.shape[0]
    tokens = packed.shape[1]
    model_width = packed.shape[2] // 3
    head_count = model_width // HEAD_DIM
    query_part = packed[:, :, :model_width].reshape(windows, tokens, head_count, HEAD_DIM)
    key_part = packed[:, :, model_width:2 * model_width].reshape(windows, tokens, head_count, HEAD_DIM)
    value_part = packed[:, :, 2 * model_width:].reshape(windows, tokens, head_count, HEAD_DIM)
    return (query_part, key_part, value_part)

def window_mask(wrap_flags, tokens):
    level_of = jnp.arange(tokens, dtype=jnp.int32) // (WIN * WIN)
    same_level = level_of[:, None] == level_of[None, :]
    allowed = jnp.logical_or(same_level[None, None], jnp.logical_not(wrap_flags)[:, None, None, None])
    return allowed.astype(jnp.float32)

def attend_forward(packed, wrap_flags):
    query_part, key_part, value_part = split_heads(packed)
    scores = jnp.einsum('wqhd,wkhd->whqk', query_part.astype(jnp.float32), key_part.astype(jnp.float32)) * HEAD_DIM ** (-0.5)
    raised = jnp.exp(scores) * window_mask(wrap_flags, packed.shape[1])
    prob = raised / lax.optimization_barrier(jnp.sum(raised, axis=-1, keepdims=True))
    prob_low = prob.astype(jnp.bfloat16)
    attended = jnp.einsum('whqk,wkhd->wqhd', prob_low.astype(jnp.float32), value_part.astype(jnp.float32))
    attended = attended.astype(jnp.bfloat16).reshape(packed.shape[0], packed.shape[1], -1)
    return (attended, prob, prob_low)

def attend_backward(packed, back_windows, prob, prob_low):
    query_part, key_part, value_part = split_heads(packed)
    back_heads = back_windows.reshape(query_part.shape).astype(jnp.float32)
    grad_value = jnp.einsum('whqk,wqhd->wkhd', prob_low.astype(jnp.float32), back_heads)
    grad_prob = jnp.einsum('wqhd,wkhd->whqk', back_heads, value_part.astype(jnp.float32))
    centre = lax.optimization_barrier(jnp.sum(prob * grad_prob, axis=-1, keepdims=True))
    grad_scores = (prob * (grad_prob - centre) * HEAD_DIM ** (-0.5)).astype(jnp.bfloat16)
    grad_query = jnp.einsum('whqk,wkhd->wqhd', grad_scores.astype(jnp.float32), key_part.astype(jnp.float32))
    grad_key = jnp.einsum('whqk,wqhd->wkhd', grad_scores.astype(jnp.float32), query_part.astype(jnp.float32))
    windows = packed.shape[0]
    tokens = packed.shape[1]
    joined = jnp.concatenate([grad_query.reshape(windows, tokens, -1), grad_key.reshape(windows, tokens, -1), grad_value.reshape(windows, tokens, -1)], axis=-1)
    return joined.astype(jnp.bfloat16)

def reference(tokens, w_qkv, w_proj, seam_codes, upstream):
    north_step = TILES // 4
    rolled_in = roll_field(tokens, seam_codes, north_step)
    rolled_up = roll_field(upstream, seam_codes, north_step)
    lev_windows = LEVELS // WIN_LEV

    def to_blocks(grid_field):
        shaped = grid_field.reshape(BATCH, lev_windows, WIN_LEV, TILES, S, S, D)
        return shaped.transpose(0, 1, 3, 2, 4, 5, 6).reshape(-1, WIN_LEV, S, S, D)

    def from_blocks(stacked):
        shaped = stacked.reshape(BATCH, lev_windows, TILES, WIN_LEV, S, S, D)
        return shaped.transpose(0, 1, 3, 2, 4, 5, 6).reshape(BATCH, LEVELS, TILES, S, S, D)
    blocks_in = to_blocks(rolled_in)
    blocks_up = to_blocks(rolled_up)
    block_count = blocks_in.shape[0]
    wrap_all = jnp.arange(block_count, dtype=jnp.int32) // TILES % lev_windows == lev_windows - 1
    contract_last = (((1,), (1,)), ((), ()))
    contract_first = (((0,), (0,)), ((), ()))

    def block_step(running, inputs):
        tokens_block, upstream_block, wrapped = inputs
        token_rows = tokens_block.reshape(-1, D)
        upstream_rows = upstream_block.reshape(-1, D)
        normalized, inverse = layer_stats(token_rows)
        hidden = normalized.astype(jnp.bfloat16)
        projected = jnp.dot(hidden, w_qkv, preferred_element_type=jnp.float32).astype(jnp.bfloat16)
        windows_qkv = to_windows(projected.reshape(WIN_LEV, S, S, 3 * D))
        wrap_flags = jnp.full((windows_qkv.shape[0],), wrapped)
        attended, prob, prob_low = attend_forward(windows_qkv, wrap_flags)
        mixed_in = from_windows(attended, WIN_LEV, S).reshape(-1, D)
        mixed_out = lax.dot_general(mixed_in, w_proj, contract_last, preferred_element_type=jnp.float32)
        output_rows = (token_rows.astype(jnp.float32) + mixed_out).astype(jnp.bfloat16)
        back_mix = jnp.dot(upstream_rows, w_proj, preferred_element_type=jnp.float32).astype(jnp.bfloat16)
        grad_windows = attend_backward(windows_qkv, to_windows(back_mix.reshape(WIN_LEV, S, S, D)), prob, prob_low)
        grad_qkv_tok = from_windows(grad_windows, WIN_LEV, S).reshape(-1, 3 * D)
        grad_hidden = lax.dot_general(grad_qkv_tok, w_qkv, contract_last, preferred_element_type=jnp.float32)
        grad_rows = norm_backward(upstream_rows, grad_hidden, normalized, inverse)
        sum_qkv = running[0] + lax.dot_general(hidden, grad_qkv_tok, contract_first, preferred_element_type=jnp.float32)
        sum_proj = running[1] + lax.dot_general(upstream_rows, mixed_in, contract_first, preferred_element_type=jnp.float32)
        return ((sum_qkv, sum_proj), (output_rows, grad_rows))
    start_sums = (jnp.zeros((D, 3 * D), jnp.float32), jnp.zeros((D, D), jnp.float32))
    sums, stacked = lax.scan(block_step, start_sums, (blocks_in, blocks_up, wrap_all))
    output = unroll_field(from_blocks(stacked[0]), seam_codes, north_step)
    grad_tokens = unroll_field(from_blocks(stacked[1]), seam_codes, north_step)
    return (output, grad_tokens, sums[0], sums[1])
```

```python
import jax
import jax.numpy as jnp
from jax import lax
from jax.sharding import PartitionSpec as P

HEAD_DIM = 32
WIN = 8
WIN_LEV = 2


EPSILON = 1e-05


def shifted(value, axis, steps):
    count = lax.axis_size(axis)
    pairs = [(source, (source + steps) % count) for source in range(count)]
    return lax.ppermute(value, axis, pairs)


def layer_stats(token_rows):
    values = token_rows.astype(jnp.float32)
    center = jnp.mean(values, axis=1, keepdims=True)
    spread = jnp.mean(jnp.square(values - center), axis=1, keepdims=True)
    inverse = lax.rsqrt(spread + EPSILON)
    return ((values - center) * inverse, inverse)


def norm_backward(upstream_rows, grad_hidden, normalized, inverse):
    centre = jnp.mean(grad_hidden, axis=1, keepdims=True)
    projected = jnp.mean(grad_hidden * normalized, axis=1, keepdims=True)
    total_grad = (
        upstream_rows.astype(jnp.float32)
        + (grad_hidden - centre - normalized * projected) * inverse
    )
    return total_grad.astype(jnp.bfloat16)


def roll_local(grid_field, east_flag, north_flag, north_step):
    shift_cells = WIN // 2
    east_part = shifted(grid_field[:, :, :shift_cells], "tile", -1)
    east_part = jnp.where(east_flag, east_part[:, ::-1], east_part)
    across = jnp.concatenate([grid_field[:, :, shift_cells:], east_part], axis=2)
    north_part = shifted(across[:, :shift_cells], "tile", -north_step)
    north_part = jnp.where(north_flag, north_part[:, :, ::-1], north_part)
    upward = jnp.concatenate([across[:, shift_cells:], north_part], axis=1)
    level_part = shifted(upward[:1], "lev", -1)
    return jnp.concatenate([upward[1:], level_part], axis=0)


def unroll_local(rolled, east_flag, north_flag, north_step):
    shift_cells = WIN // 2
    extent = rolled.shape[1]
    level_part = shifted(rolled[-1:], "lev", 1)
    upward = jnp.concatenate([level_part, rolled[:-1]], axis=0)
    north_part = upward[:, extent - shift_cells :]
    north_part = jnp.where(north_flag, north_part[:, :, ::-1], north_part)
    north_part = shifted(north_part, "tile", north_step)
    across = jnp.concatenate([north_part, upward[:, : extent - shift_cells]], axis=1)
    east_part = across[:, :, extent - shift_cells :]
    east_part = jnp.where(east_flag, east_part[:, ::-1], east_part)
    east_part = shifted(east_part, "tile", 1)
    return jnp.concatenate([east_part, across[:, :, : extent - shift_cells]], axis=2)


def to_windows(grid_field):
    levels = grid_field.shape[0]
    extent = grid_field.shape[1]
    channels = grid_field.shape[3]
    blocks = grid_field.reshape(
        levels // WIN_LEV, WIN_LEV, extent // WIN, WIN, extent // WIN, WIN, channels
    )
    blocks = blocks.transpose(0, 2, 4, 1, 3, 5, 6)
    return blocks.reshape(-1, WIN_LEV * WIN * WIN, channels)


def from_windows(windows, levels, extent):
    channels = windows.shape[-1]
    blocks = windows.reshape(
        levels // WIN_LEV, extent // WIN, extent // WIN, WIN_LEV, WIN, WIN, channels
    )
    blocks = blocks.transpose(0, 3, 1, 4, 2, 5, 6)
    return blocks.reshape(levels, extent, extent, channels)


def split_heads(packed):
    windows = packed.shape[0]
    tokens = packed.shape[1]
    model_width = packed.shape[2] // 3
    head_count = model_width // HEAD_DIM
    query_part = packed[:, :, :model_width].reshape(windows, tokens, head_count, HEAD_DIM)
    key_part = packed[:, :, model_width : 2 * model_width].reshape(
        windows, tokens, head_count, HEAD_DIM
    )
    value_part = packed[:, :, 2 * model_width :].reshape(windows, tokens, head_count, HEAD_DIM)
    return (query_part, key_part, value_part)


def window_mask(wrap_flags, tokens):
    level_of = jnp.arange(tokens, dtype=jnp.int32) // (WIN * WIN)
    same_level = level_of[:, None] == level_of[None, :]
    allowed = jnp.logical_or(
        same_level[None, None], jnp.logical_not(wrap_flags)[:, None, None, None]
    )
    return allowed.astype(jnp.float32)


def attend_forward(packed, wrap_flags):
    query_part, key_part, value_part = split_heads(packed)
    scores = jnp.einsum(
        "wqhd,wkhd->whqk", query_part, key_part, preferred_element_type=jnp.float32
    ) * HEAD_DIM ** (-0.5)
    raised = jnp.exp(scores) * window_mask(wrap_flags, packed.shape[1])
    prob = raised / jnp.sum(raised, axis=-1, keepdims=True)
    prob_low = prob.astype(jnp.bfloat16)
    attended = jnp.einsum(
        "whqk,wkhd->wqhd", prob_low, value_part, preferred_element_type=jnp.float32
    )
    attended = attended.astype(jnp.bfloat16).reshape(packed.shape[0], packed.shape[1], -1)
    return (attended, prob, prob_low)


def attend_backward(packed, back_windows, prob, prob_low):
    query_part, key_part, value_part = split_heads(packed)
    back_heads = back_windows.reshape(query_part.shape)
    grad_value = jnp.einsum(
        "whqk,wqhd->wkhd", prob_low, back_heads, preferred_element_type=jnp.float32
    )
    grad_prob = jnp.einsum(
        "wqhd,wkhd->whqk", back_heads, value_part, preferred_element_type=jnp.float32
    )
    centre = jnp.sum(prob * grad_prob, axis=-1, keepdims=True)
    grad_scores = (prob * (grad_prob - centre) * HEAD_DIM ** (-0.5)).astype(jnp.bfloat16)
    grad_query = jnp.einsum(
        "whqk,wkhd->wqhd", grad_scores, key_part, preferred_element_type=jnp.float32
    )
    grad_key = jnp.einsum(
        "whqk,wqhd->wkhd", grad_scores, query_part, preferred_element_type=jnp.float32
    )
    windows = packed.shape[0]
    tokens = packed.shape[1]
    joined = jnp.concatenate(
        [
            grad_query.reshape(windows, tokens, -1),
            grad_key.reshape(windows, tokens, -1),
            grad_value.reshape(windows, tokens, -1),
        ],
        axis=-1,
    )
    return joined.astype(jnp.bfloat16)


def shards_general(tokens, w_qkv, w_proj, seam_codes, upstream):
    levels = tokens.shape[1]
    extent = tokens.shape[3]
    model_width = tokens.shape[5]
    tiles_count = lax.axis_size("tile")
    north_step = tiles_count // 4
    tile_here = lax.axis_index("tile")
    east_flag = seam_codes[tile_here, 0] == 1
    north_flag = seam_codes[tile_here, 1] == 1
    top_level = lax.axis_index("lev") == lax.axis_size("lev") - 1
    per_level = extent // WIN * (extent // WIN)
    window_total = levels // WIN_LEV * per_level
    lev_window = jnp.arange(window_total, dtype=jnp.int32) // per_level
    wrap_flags = jnp.logical_and(top_level, lev_window == levels // WIN_LEV - 1)
    contract_last = (((1,), (1,)), ((), ()))
    contract_first = (((0,), (0,)), ((), ()))
    grid_in = tokens.reshape(levels, extent, extent, model_width)
    grid_up = upstream.reshape(levels, extent, extent, model_width)
    paired = roll_local(
        jnp.concatenate([grid_in, grid_up], axis=-1), east_flag, north_flag, north_step
    )
    grid_in = paired[..., :model_width]
    grid_up = paired[..., model_width:]
    token_rows = grid_in.reshape(-1, model_width)
    upstream_rows = grid_up.reshape(-1, model_width)
    normalized, inverse = layer_stats(token_rows)
    hidden = normalized.astype(jnp.bfloat16)
    full_qkv, full_proj = (
        lax.all_gather(w_qkv, "tile", axis=0, tiled=True),
        lax.all_gather(w_proj, "tile", axis=0, tiled=True),
    )
    projected = jnp.dot(hidden, full_qkv, preferred_element_type=jnp.float32).astype(jnp.bfloat16)
    grid_qkv = projected.reshape(levels, extent, extent, 3 * model_width)
    windows_qkv = to_windows(grid_qkv)
    attended, prob, prob_low = attend_forward(windows_qkv, wrap_flags)
    grid_mixed = from_windows(attended, levels, extent)
    mixed_in = grid_mixed.reshape(-1, model_width)
    mixed_out = lax.dot_general(
        mixed_in, full_proj, contract_last, preferred_element_type=jnp.float32
    )
    back_mix = jnp.dot(upstream_rows, full_proj, preferred_element_type=jnp.float32)
    output_low = (token_rows.astype(jnp.float32) + mixed_out).astype(jnp.bfloat16)
    back_low = back_mix.astype(jnp.bfloat16)
    grid_back = back_low.reshape(levels, extent, extent, model_width)
    grad_windows = attend_backward(windows_qkv, to_windows(grid_back), prob, prob_low)
    grid_grad = from_windows(grad_windows, levels, extent)
    grad_qkv_tok = grid_grad.reshape(-1, 3 * model_width)
    grad_hidden = lax.dot_general(
        grad_qkv_tok, full_qkv, contract_last, preferred_element_type=jnp.float32
    )
    grad_low = norm_backward(upstream_rows, grad_hidden, normalized, inverse)
    grid_output = output_low.reshape(levels, extent, extent, model_width)
    grid_dx = grad_low.reshape(levels, extent, extent, model_width)
    paired = unroll_local(
        jnp.concatenate([grid_output, grid_dx], axis=-1), east_flag, north_flag, north_step
    )
    grid_output = paired[..., :model_width]
    grid_dx = paired[..., model_width:]
    columns = hidden
    share_qkv = lax.psum_scatter(
        lax.dot_general(
            columns, grad_qkv_tok, contract_first, preferred_element_type=jnp.float32
        ).astype(jnp.bfloat16),
        "tile",
        scatter_dimension=0,
        tiled=True,
    )
    columns = upstream_rows
    share_proj = lax.psum_scatter(
        lax.dot_general(
            columns, mixed_in, contract_first, preferred_element_type=jnp.float32
        ).astype(jnp.bfloat16),
        "tile",
        scatter_dimension=0,
        tiled=True,
    )
    grad_qkv, grad_proj = (
        lax.psum(share_qkv, ("rep", "lev")).astype(jnp.float32),
        lax.psum(share_proj, ("rep", "lev")).astype(jnp.float32),
    )
    return (grid_output.reshape(tokens.shape), grid_dx.reshape(tokens.shape), grad_qkv, grad_proj)


def swapped(value, axis, mask):
    count = lax.axis_size(axis)
    return lax.ppermute(value, axis, [(source, source ^ mask) for source in range(count)])


def roll_selector(seam_codes, tile_here, tiles_count, extent):
    half = WIN // 2
    north_step = tiles_count // 4
    slot = jnp.arange(tiles_count, dtype=jnp.int32)[:, None, None]
    row = jnp.arange(extent, dtype=jnp.int32)[None, :, None]
    col = jnp.arange(extent, dtype=jnp.int32)[None, None, :]

    def code_of(tile, which):
        found = jnp.zeros_like(tile)
        for t in range(tiles_count):
            found = jnp.where(tile == t, seam_codes[t, which], found)
        return found == 1

    tile = jnp.bitwise_xor(slot, tile_here)
    crossed = row >= extent - half
    col1 = jnp.where(crossed & code_of(tile, 1), extent - 1 - col, col)
    row1 = jnp.where(crossed, row - (extent - half), row + half)
    tile1 = jnp.where(crossed, (tile + north_step) % tiles_count, tile)
    crossed = col1 >= extent - half
    row2 = jnp.where(crossed & code_of(tile1, 0), extent - 1 - row1, row1)
    col2 = jnp.where(crossed, col1 - (extent - half), col1 + half)
    tile2 = jnp.where(crossed, (tile1 + 1) % tiles_count, tile1)
    source = (jnp.bitwise_xor(tile2, tile_here) * extent + row2) * extent + col2
    source = source.reshape(-1, 1)
    cells = source.shape[0]
    return (source == jnp.arange(cells, dtype=jnp.int32)[None, :]).astype(jnp.bfloat16)


def cat_dot(a, b, dims):
    return lax.dot_general(a, b, (dims, ((), ())), preferred_element_type=jnp.float32)


def local_math(tokens_all, upstream_all, w_heads, w_out, selector, wrapped):
    levels, cells, channels = tokens_all.shape
    own = w_out.shape[1]
    heads = own // HEAD_DIM
    side = WIN * WIN
    windows = cells // side

    def rolled(rows):
        out = jnp.einsum("rs,lsc->lrc", selector, rows.reshape(levels, cells, -1), preferred_element_type=jnp.float32)
        return out.astype(jnp.bfloat16)

    def unrolled(rows):
        out = jnp.einsum("rs,lrc->lsc", selector, rows, preferred_element_type=jnp.float32)
        return out.astype(jnp.bfloat16).reshape(levels * cells, -1)

    def windowed(rows):
        return rows.reshape(levels, windows, side, -1).transpose(1, 0, 2, 3).reshape(windows, levels * side, -1)

    def unwindowed(blocks):
        return blocks.reshape(windows, levels, side, -1).transpose(1, 0, 2, 3).reshape(levels, cells, -1)

    normalized, inverse = layer_stats(tokens_all.reshape(-1, channels))
    hidden = normalized.astype(jnp.bfloat16)
    up_rows = upstream_all.reshape(-1, channels)
    qkv = jnp.dot(hidden, w_heads, preferred_element_type=jnp.float32).astype(jnp.bfloat16)
    packed = windowed(rolled(qkv))
    flags = jnp.full((windows,), wrapped)
    attended, prob, prob_low = attend_forward(packed, flags)
    mixed_in = unrolled(unwindowed(attended))
    back = jnp.dot(up_rows, w_out, preferred_element_type=jnp.float32).astype(jnp.bfloat16)
    back_windows = windowed(rolled(back))
    grads = attend_backward(packed, back_windows, prob, prob_low)
    grad_tok = unrolled(unwindowed(grads))
    mixed_out = cat_dot(mixed_in, w_out, ((1,), (1,))).astype(jnp.bfloat16)
    grad_hidden = cat_dot(grad_tok, w_heads, ((1,), (1,))).astype(jnp.bfloat16)
    share = cat_dot(hidden, grad_tok, ((0,), (0,))).astype(jnp.bfloat16)
    share_out = cat_dot(up_rows, mixed_in, ((0,), (0,))).astype(jnp.bfloat16)
    sums = jnp.concatenate([mixed_out, grad_hidden], axis=-1).reshape(levels, cells, 2 * channels)
    share_a = share[:, : 2 * own]
    share_b = jnp.concatenate([share[:, 2 * own :], share_out], axis=1)
    return sums, share_a, share_b


def reduce_share(share, rep_here, lev_here, tile_here):
    tiles_count, reps, levs = lax.axis_size("tile"), lax.axis_size("rep"), lax.axis_size("lev")
    cols = share.shape[1]
    part = share.reshape(tiles_count, reps, -1, cols)
    for mask in range(1, reps):
        pass
    mine = lax.dynamic_index_in_dim(part, rep_here, 1, keepdims=False)
    total = mine.astype(jnp.float32)
    for mask in range(1, reps):
        away = lax.dynamic_index_in_dim(part, rep_here ^ mask, 1, keepdims=False)
        total = total + swapped(away, "rep", mask).astype(jnp.float32)
    part = total.astype(jnp.bfloat16).reshape(tiles_count, levs, -1, cols)
    total = lax.dynamic_index_in_dim(part, lev_here, 1, keepdims=False).astype(jnp.float32)
    for mask in range(1, levs):
        away = lax.dynamic_index_in_dim(part, lev_here ^ mask, 1, keepdims=False)
        total = total + swapped(away, "lev", mask).astype(jnp.float32)
    part = total.astype(jnp.bfloat16)
    slots = [lax.dynamic_index_in_dim(part, tile_here, 0, keepdims=False)]
    for mask in range(1, tiles_count):
        slots.append(swapped(lax.dynamic_index_in_dim(part, tile_here ^ mask, 0, keepdims=False), "tile", mask))
    return jnp.stack(in_order(slots, tile_here))


def in_order(slots, here):
    bit = 1
    while bit < len(slots):
        odd = jnp.bitwise_and(here, bit) != 0
        slots = [jnp.where(odd, slots[k ^ bit], slots[k]) for k in range(len(slots))]
        bit *= 2
    return slots


def spread(piece, axis, here):
    count = lax.axis_size(axis)
    slots = [piece] + [swapped(piece, axis, mask) for mask in range(1, count)]
    return jnp.concatenate(in_order(slots, here), axis=0)


def shards_by_heads(tokens, w_qkv, w_proj, seam_codes, upstream):
    levels, extent, channels = tokens.shape[1], tokens.shape[3], tokens.shape[5]
    cells = extent * extent
    tiles_count = lax.axis_size("tile")
    rep_here, lev_here, tile_here = lax.axis_index("rep"), lax.axis_index("lev"), lax.axis_index("tile")
    own = channels // tiles_count
    shard_rows = w_qkv.shape[0]
    wrapped = lev_here == lax.axis_size("lev") - 1
    field_in = tokens.reshape(levels, cells, channels)
    field_up = upstream.reshape(levels, cells, channels)

    def dealt(blocks):
        slots = [lax.dynamic_index_in_dim(blocks, tile_here, 2, keepdims=False)]
        for mask in range(1, tiles_count):
            slots.append(swapped(lax.dynamic_index_in_dim(blocks, tile_here ^ mask, 2, keepdims=False).reshape(shard_rows, -1), "tile", mask))
        slots[0] = slots[0].reshape(shard_rows, -1)
        return jnp.concatenate(in_order(slots, tile_here), axis=0)

    blocks_qkv = w_qkv.reshape(shard_rows, 3, tiles_count, own)
    blocks_out = w_proj.reshape(shard_rows, 1, tiles_count, own)
    w_a = dealt(blocks_qkv[:, :2])
    w_b = dealt(jnp.concatenate([blocks_qkv[:, 2:], blocks_out], axis=1))
    w_heads = jnp.concatenate([w_a, w_b[:, :own]], axis=1)
    w_out = w_b[:, own:]

    def gathered(piece):
        slots = [piece]
        bit = 1
        while bit < tiles_count:
            bit *= 2
        bit //= 2
        have = {0: piece}
        while bit:
            for k in list(have):
                have[k ^ bit] = swapped(have[k], "tile", bit)
            bit //= 2
        return jnp.concatenate([have[k] for k in range(tiles_count)], axis=0)

    both = jnp.concatenate([field_in, field_up], axis=-1)
    low = shifted(both[0], "lev", -1)
    high_all = gathered(both[1])
    low_all = gathered(low)
    both_all = jnp.stack([high_all, low_all])
    selector = roll_selector(seam_codes, tile_here, tiles_count, extent)
    sums, share_a, share_b = local_math(
        both_all[..., :channels], both_all[..., channels:], w_heads, w_out, selector, wrapped
    )

    sums = sums.reshape(levels, tiles_count, cells, 2 * channels)
    have = [sums[:, k] for k in range(tiles_count)]
    bit = 1
    while bit < tiles_count:
        away = jnp.stack([have[k] for k in range(1, len(have), 2)])
        came = swapped(away, "tile", bit)
        have = [
            (have[2 * k].astype(jnp.float32) + came[k].astype(jnp.float32)).astype(jnp.bfloat16)
            for k in range(len(have) // 2)
        ]
        bit *= 2
    final = have[0]
    low_back = shifted(final[1], "lev", 1)
    final = jnp.stack([low_back, final[0]]).reshape(levels * cells, 2 * channels)
    token_rows = field_in.reshape(-1, channels)
    upstream_rows = field_up.reshape(-1, channels)
    normalized, inverse = layer_stats(token_rows)
    output = (token_rows.astype(jnp.float32) + final[:, :channels].astype(jnp.float32)).astype(jnp.bfloat16)
    grad_tokens = norm_backward(upstream_rows, final[:, channels:].astype(jnp.float32), normalized, inverse)

    grads = []
    for share in (share_b, share_a):
        piece = reduce_share(share, rep_here, lev_here, tile_here)
        rows = piece.shape[1]
        piece = piece.reshape(tiles_count, rows, 2, own).transpose(1, 2, 0, 3).reshape(rows, 2 * channels)
        piece = spread(piece, "lev", lev_here)
        grads.append(spread(piece, "rep", rep_here).astype(jnp.float32))
    grad_b, grad_a = grads
    grad_qkv = jnp.concatenate([grad_a, grad_b[:, :channels]], axis=1)
    grad_proj = grad_b[:, channels:]
    return (output.reshape(tokens.shape), grad_tokens.reshape(tokens.shape), grad_qkv, grad_proj)


def power_of_two(count):
    return count & (count - 1) == 0


def shards(tokens, w_qkv, w_proj, seam_codes, upstream):
    counts = [lax.axis_size(axis) for axis in ("rep", "lev", "tile")]
    tiles_count = counts[2]
    channels = tokens.shape[5]
    one_window = tokens.shape[0] == 1 and tokens.shape[1] == WIN_LEV and tokens.shape[3] == WIN and tokens.shape[2] == 1
    by_heads = (
        one_window
        and all(power_of_two(count) for count in counts)
        and tiles_count % 4 == 0
        and (channels // HEAD_DIM) % tiles_count == 0
        and (channels // tiles_count) % (counts[0] * counts[1]) == 0
    )
    body = shards_by_heads if by_heads else shards_general
    return body(tokens, w_qkv, w_proj, seam_codes, upstream)


def solution(mesh):
    in_specs = (
        P("rep", "lev", "tile", None, None, None),
        P("tile", None),
        P("tile", None),
        P(),
        P("rep", "lev", "tile", None, None, None),
    )
    out_specs = (
        P("rep", "lev", "tile", None, None, None),
        P("rep", "lev", "tile", None, None, None),
        P("tile", None),
        P("tile", None),
    )
    return jax.shard_map(shards, mesh=mesh, in_specs=in_specs, out_specs=out_specs, check_vma=False)
```

```python
import jax
import jax.numpy as jnp
from jax import lax
from jax.experimental import pallas as pl
from jax.experimental.pallas import tpu as pltpu
from jax.sharding import PartitionSpec as P

HEAD_DIM = 32
WIN = 8
WIN_LEV = 2


EPSILON = 1e-05


def shifted(value, axis, steps):
    count = lax.axis_size(axis)
    pairs = [(source, (source + steps) % count) for source in range(count)]
    return lax.ppermute(value, axis, pairs)


def layer_stats(token_rows):
    values = token_rows.astype(jnp.float32)
    center = jnp.mean(values, axis=1, keepdims=True)
    spread = jnp.mean(jnp.square(values - center), axis=1, keepdims=True)
    inverse = lax.rsqrt(spread + EPSILON)
    return ((values - center) * inverse, inverse)


def norm_backward(upstream_rows, grad_hidden, normalized, inverse):
    centre = jnp.mean(grad_hidden, axis=1, keepdims=True)
    projected = jnp.mean(grad_hidden * normalized, axis=1, keepdims=True)
    total_grad = (
        upstream_rows.astype(jnp.float32)
        + (grad_hidden - centre - normalized * projected) * inverse
    )
    return total_grad.astype(jnp.bfloat16)


def roll_local(grid_field, east_flag, north_flag, north_step):
    shift_cells = WIN // 2
    east_part = shifted(grid_field[:, :, :shift_cells], "tile", -1)
    east_part = jnp.where(east_flag, east_part[:, ::-1], east_part)
    across = jnp.concatenate([grid_field[:, :, shift_cells:], east_part], axis=2)
    north_part = shifted(across[:, :shift_cells], "tile", -north_step)
    north_part = jnp.where(north_flag, north_part[:, :, ::-1], north_part)
    upward = jnp.concatenate([across[:, shift_cells:], north_part], axis=1)
    level_part = shifted(upward[:1], "lev", -1)
    return jnp.concatenate([upward[1:], level_part], axis=0)


def unroll_local(rolled, east_flag, north_flag, north_step):
    shift_cells = WIN // 2
    extent = rolled.shape[1]
    level_part = shifted(rolled[-1:], "lev", 1)
    upward = jnp.concatenate([level_part, rolled[:-1]], axis=0)
    north_part = upward[:, extent - shift_cells :]
    north_part = jnp.where(north_flag, north_part[:, :, ::-1], north_part)
    north_part = shifted(north_part, "tile", north_step)
    across = jnp.concatenate([north_part, upward[:, : extent - shift_cells]], axis=1)
    east_part = across[:, :, extent - shift_cells :]
    east_part = jnp.where(east_flag, east_part[:, ::-1], east_part)
    east_part = shifted(east_part, "tile", 1)
    return jnp.concatenate([east_part, across[:, :, : extent - shift_cells]], axis=2)


def to_windows(grid_field):
    levels = grid_field.shape[0]
    extent = grid_field.shape[1]
    channels = grid_field.shape[3]
    blocks = grid_field.reshape(
        levels // WIN_LEV, WIN_LEV, extent // WIN, WIN, extent // WIN, WIN, channels
    )
    blocks = blocks.transpose(0, 2, 4, 1, 3, 5, 6)
    return blocks.reshape(-1, WIN_LEV * WIN * WIN, channels)


def from_windows(windows, levels, extent):
    channels = windows.shape[-1]
    blocks = windows.reshape(
        levels // WIN_LEV, extent // WIN, extent // WIN, WIN_LEV, WIN, WIN, channels
    )
    blocks = blocks.transpose(0, 3, 1, 4, 2, 5, 6)
    return blocks.reshape(levels, extent, extent, channels)


def split_heads(packed):
    windows = packed.shape[0]
    tokens = packed.shape[1]
    model_width = packed.shape[2] // 3
    head_count = model_width // HEAD_DIM
    query_part = packed[:, :, :model_width].reshape(windows, tokens, head_count, HEAD_DIM)
    key_part = packed[:, :, model_width : 2 * model_width].reshape(
        windows, tokens, head_count, HEAD_DIM
    )
    value_part = packed[:, :, 2 * model_width :].reshape(windows, tokens, head_count, HEAD_DIM)
    return (query_part, key_part, value_part)


def window_mask(wrap_flags, tokens):
    level_of = jnp.arange(tokens, dtype=jnp.int32) // (WIN * WIN)
    same_level = level_of[:, None] == level_of[None, :]
    allowed = jnp.logical_or(
        same_level[None, None], jnp.logical_not(wrap_flags)[:, None, None, None]
    )
    return allowed.astype(jnp.float32)


def attend_forward(packed, wrap_flags):
    query_part, key_part, value_part = split_heads(packed)
    scores = jnp.einsum(
        "wqhd,wkhd->whqk", query_part, key_part, preferred_element_type=jnp.float32
    ) * HEAD_DIM ** (-0.5)
    raised = jnp.exp(scores) * window_mask(wrap_flags, packed.shape[1])
    prob = raised / jnp.sum(raised, axis=-1, keepdims=True)
    prob_low = prob.astype(jnp.bfloat16)
    attended = jnp.einsum(
        "whqk,wkhd->wqhd", prob_low, value_part, preferred_element_type=jnp.float32
    )
    attended = attended.astype(jnp.bfloat16).reshape(packed.shape[0], packed.shape[1], -1)
    return (attended, prob, prob_low)


def attend_backward(packed, back_windows, prob, prob_low):
    query_part, key_part, value_part = split_heads(packed)
    back_heads = back_windows.reshape(query_part.shape)
    grad_value = jnp.einsum(
        "whqk,wqhd->wkhd", prob_low, back_heads, preferred_element_type=jnp.float32
    )
    grad_prob = jnp.einsum(
        "wqhd,wkhd->whqk", back_heads, value_part, preferred_element_type=jnp.float32
    )
    centre = jnp.sum(prob * grad_prob, axis=-1, keepdims=True)
    grad_scores = (prob * (grad_prob - centre) * HEAD_DIM ** (-0.5)).astype(jnp.bfloat16)
    grad_query = jnp.einsum(
        "whqk,wkhd->wqhd", grad_scores, key_part, preferred_element_type=jnp.float32
    )
    grad_key = jnp.einsum(
        "whqk,wqhd->wkhd", grad_scores, query_part, preferred_element_type=jnp.float32
    )
    windows = packed.shape[0]
    tokens = packed.shape[1]
    joined = jnp.concatenate(
        [
            grad_query.reshape(windows, tokens, -1),
            grad_key.reshape(windows, tokens, -1),
            grad_value.reshape(windows, tokens, -1),
        ],
        axis=-1,
    )
    return joined.astype(jnp.bfloat16)


def shards_general(tokens, w_qkv, w_proj, seam_codes, upstream):
    levels = tokens.shape[1]
    extent = tokens.shape[3]
    model_width = tokens.shape[5]
    tiles_count = lax.axis_size("tile")
    north_step = tiles_count // 4
    tile_here = lax.axis_index("tile")
    east_flag = seam_codes[tile_here, 0] == 1
    north_flag = seam_codes[tile_here, 1] == 1
    top_level = lax.axis_index("lev") == lax.axis_size("lev") - 1
    per_level = extent // WIN * (extent // WIN)
    window_total = levels // WIN_LEV * per_level
    lev_window = jnp.arange(window_total, dtype=jnp.int32) // per_level
    wrap_flags = jnp.logical_and(top_level, lev_window == levels // WIN_LEV - 1)
    contract_last = (((1,), (1,)), ((), ()))
    contract_first = (((0,), (0,)), ((), ()))
    grid_in = tokens.reshape(levels, extent, extent, model_width)
    grid_up = upstream.reshape(levels, extent, extent, model_width)
    paired = roll_local(
        jnp.concatenate([grid_in, grid_up], axis=-1), east_flag, north_flag, north_step
    )
    grid_in = paired[..., :model_width]
    grid_up = paired[..., model_width:]
    token_rows = grid_in.reshape(-1, model_width)
    upstream_rows = grid_up.reshape(-1, model_width)
    normalized, inverse = layer_stats(token_rows)
    hidden = normalized.astype(jnp.bfloat16)
    full_qkv, full_proj = (
        lax.all_gather(w_qkv, "tile", axis=0, tiled=True),
        lax.all_gather(w_proj, "tile", axis=0, tiled=True),
    )
    projected = jnp.dot(hidden, full_qkv, preferred_element_type=jnp.float32).astype(jnp.bfloat16)
    grid_qkv = projected.reshape(levels, extent, extent, 3 * model_width)
    windows_qkv = to_windows(grid_qkv)
    attended, prob, prob_low = attend_forward(windows_qkv, wrap_flags)
    grid_mixed = from_windows(attended, levels, extent)
    mixed_in = grid_mixed.reshape(-1, model_width)
    mixed_out = lax.dot_general(
        mixed_in, full_proj, contract_last, preferred_element_type=jnp.float32
    )
    back_mix = jnp.dot(upstream_rows, full_proj, preferred_element_type=jnp.float32)
    output_low = (token_rows.astype(jnp.float32) + mixed_out).astype(jnp.bfloat16)
    back_low = back_mix.astype(jnp.bfloat16)
    grid_back = back_low.reshape(levels, extent, extent, model_width)
    grad_windows = attend_backward(windows_qkv, to_windows(grid_back), prob, prob_low)
    grid_grad = from_windows(grad_windows, levels, extent)
    grad_qkv_tok = grid_grad.reshape(-1, 3 * model_width)
    grad_hidden = lax.dot_general(
        grad_qkv_tok, full_qkv, contract_last, preferred_element_type=jnp.float32
    )
    grad_low = norm_backward(upstream_rows, grad_hidden, normalized, inverse)
    grid_output = output_low.reshape(levels, extent, extent, model_width)
    grid_dx = grad_low.reshape(levels, extent, extent, model_width)
    paired = unroll_local(
        jnp.concatenate([grid_output, grid_dx], axis=-1), east_flag, north_flag, north_step
    )
    grid_output = paired[..., :model_width]
    grid_dx = paired[..., model_width:]
    columns = hidden
    share_qkv = lax.psum_scatter(
        lax.dot_general(
            columns, grad_qkv_tok, contract_first, preferred_element_type=jnp.float32
        ).astype(jnp.bfloat16),
        "tile",
        scatter_dimension=0,
        tiled=True,
    )
    columns = upstream_rows
    share_proj = lax.psum_scatter(
        lax.dot_general(
            columns, mixed_in, contract_first, preferred_element_type=jnp.float32
        ).astype(jnp.bfloat16),
        "tile",
        scatter_dimension=0,
        tiled=True,
    )
    grad_qkv, grad_proj = (
        lax.psum(share_qkv, ("rep", "lev")).astype(jnp.float32),
        lax.psum(share_proj, ("rep", "lev")).astype(jnp.float32),
    )
    return (grid_output.reshape(tokens.shape), grid_dx.reshape(tokens.shape), grad_qkv, grad_proj)


LANES = 128
NEAR = LANES // HEAD_DIM


def swapped(value, axis, mask):
    count = lax.axis_size(axis)
    return lax.ppermute(value, axis, [(source, source ^ mask) for source in range(count)])


def roll_source(seam_codes, tile_here, tiles_count, extent):
    half = WIN // 2
    north_step = tiles_count // 4
    slot = jnp.arange(tiles_count, dtype=jnp.int32)[:, None, None]
    row = jnp.arange(extent, dtype=jnp.int32)[None, :, None]
    col = jnp.arange(extent, dtype=jnp.int32)[None, None, :]

    def code_of(tile, which):
        found = jnp.zeros_like(tile)
        for t in range(tiles_count):
            found = jnp.where(tile == t, seam_codes[t, which], found)
        return found == 1

    tile = jnp.bitwise_xor(slot, tile_here)
    crossed = row >= extent - half
    col1 = jnp.where(crossed & code_of(tile, 1), extent - 1 - col, col)
    row1 = jnp.where(crossed, row - (extent - half), row + half)
    tile1 = jnp.where(crossed, (tile + north_step) % tiles_count, tile)
    crossed = col1 >= extent - half
    row2 = jnp.where(crossed & code_of(tile1, 0), extent - 1 - row1, row1)
    col2 = jnp.where(crossed, col1 - (extent - half), col1 + half)
    tile2 = jnp.where(crossed, (tile1 + 1) % tiles_count, tile1)
    source = (jnp.bitwise_xor(tile2, tile_here) * extent + row2) * extent + col2
    return source.reshape(-1)


def in_order(slots, here):
    bit = 1
    while bit < len(slots):
        odd = jnp.bitwise_and(here, bit) != 0
        slots = [jnp.where(odd, slots[k ^ bit], slots[k]) for k in range(len(slots))]
        bit *= 2
    return slots


def dot_nn(a, b):
    return lax.dot_general(a, b, (((1,), (0,)), ((), ())), preferred_element_type=jnp.float32)


def dot_nt(a, b):
    return lax.dot_general(a, b, (((1,), (1,)), ((), ())), preferred_element_type=jnp.float32)


def dot_tn(a, b):
    return lax.dot_general(a, b, (((0,), (0,)), ((), ())), preferred_element_type=jnp.float32)


def deal_kernel(here_ref, qkv_ref, out_ref, *block_refs):
    tiles_count = len(block_refs)
    channels = out_ref.shape[1]
    own = channels // tiles_count
    here = here_ref[0]

    def columns(which, tile):
        ref = out_ref if which == 3 else qkv_ref
        base = (0 if which == 3 else which * channels) + tile * own
        return ref[:, base : base + LANES], ref[:, base + LANES : base + own]

    blocks = []
    for tile in range(tiles_count):
        (q, q1), (k, k1), (v, v1), (p, p1) = [columns(which, tile) for which in range(4)]
        blocks.append(jnp.concatenate([q, k, q1, k1, v, p, v1, p1], axis=1))
    for ref, block in zip(block_refs, in_order(blocks, here)):
        ref[...] = block


def attend_window(block, allowed):
    tokens = block.shape[0]
    lane = lax.broadcasted_iota(jnp.int32, (1, LANES), 1)
    group = [block[:, g * LANES : (g + 1) * LANES] for g in range(6)]
    scale = HEAD_DIM ** (-0.5)

    def turned(x):
        return pltpu.roll(x.astype(jnp.float32), LANES // 2, 1)

    def attend(q, k, v, o, heads):
        masks = [lane // HEAD_DIM == h for h in range(heads)]

        def stacked(x):
            return jnp.concatenate([jnp.where(m, x, jnp.zeros_like(x)) for m in masks], axis=0)

        def folded(x):
            total = jnp.where(masks[0], x[:tokens], 0.0)
            for h in range(1, heads):
                total = jnp.where(masks[h], x[h * tokens : (h + 1) * tokens], total)
            return total

        k_all, v_all = stacked(k), stacked(v)
        scores = (dot_nt(k_all, q) * scale).reshape(heads, tokens, tokens)
        raised = jnp.exp(scores) * allowed[None]
        prob = raised / jnp.sum(raised, axis=1, keepdims=True)
        grad_prob = dot_nt(v_all, o).reshape(heads, tokens, tokens)
        centre = jnp.sum(prob * grad_prob, axis=1, keepdims=True)
        grad_scores = (prob * (grad_prob - centre) * scale).astype(jnp.bfloat16).reshape(-1, tokens)
        prob_low = prob.astype(jnp.bfloat16).reshape(-1, tokens)
        att = dot_tn(prob_low, v_all)
        grad_q = dot_tn(grad_scores, k_all)
        grad_k = folded(dot_nn(grad_scores, q))
        grad_v = folded(dot_nn(prob_low, o))
        return grad_q, grad_k, grad_v, att

    gq, gk, gv, att = attend(group[0], group[1], group[3], group[4], NEAR)
    qk_turned = turned(group[2]).astype(jnp.bfloat16)
    vo_turned = turned(group[5]).astype(jnp.bfloat16)
    gq1, gk1, gv1, att1 = attend(group[2], qk_turned, group[5], vo_turned, NEAR // 2)
    parts = [gq, gk, gq1 + turned(gk1), gv, att, gv1 + turned(att1)]
    return jnp.concatenate(parts, axis=1).astype(jnp.bfloat16)


def main_kernel(
    scal_ref, from_col_ref, from_row_ref, *refs
):
    tiles_count = (len(refs) - 6 - 5) // 3
    cells_refs = refs[: 2 * tiles_count]
    block_refs = refs[2 * tiles_count : 3 * tiles_count]
    keep_ref, send_ref, keep_a, send_a, keep_b, send_b = refs[3 * tiles_count : 3 * tiles_count + 6]
    hid, up, wts, rolled, result = refs[3 * tiles_count + 6 :]
    cells = cells_refs[0].shape[0]
    channels = wts.shape[0]
    rows = channels // tiles_count
    plane = tiles_count * cells
    wrapped, rep, here = scal_ref[0], scal_ref[1], scal_ref[2]
    for k in range(tiles_count):
        wts[pl.ds(pl.multiple_of((here ^ k) * rows, 64), rows), :] = block_refs[k][...]
    for k in range(tiles_count):
        for l in range(2):
            at = l * plane + k * cells
            x = cells_refs[2 * k + l][:, :channels].astype(jnp.float32)
            center = jnp.mean(x, axis=1, keepdims=True)
            x = x - center
            spread = jnp.mean(jnp.square(x), axis=1, keepdims=True)
            hid[at : at + cells, :] = (x * lax.rsqrt(spread + EPSILON)).astype(jnp.bfloat16)
            up[at : at + cells, :] = cells_refs[2 * k + l][:, channels:]

    lane = lax.broadcasted_iota(jnp.int32, (1, LANES), 1)
    low = lane < LANES // 2
    split = 4 * LANES
    from_col = lax.broadcasted_iota(jnp.int32, (plane, plane), 1) == from_col_ref[...]
    selector = jnp.where(from_col, 1.0, 0.0).astype(jnp.bfloat16)
    from_row = lax.broadcasted_iota(jnp.int32, (plane, plane), 0) == from_row_ref[...]
    back_selector = jnp.where(from_row, 1.0, 0.0).astype(jnp.bfloat16)
    for l in range(2):
        at = slice(l * plane, (l + 1) * plane)
        front = dot_nn(hid[at, :], wts[:, :split])
        last = dot_nn(hid[at, :], wts[:, split + LANES :])
        back = dot_nn(up[at, :], wts[:, split:])
        mixed = jnp.where(low, last, back[:, LANES:])
        whole = jnp.concatenate([front, back[:, :LANES], mixed], axis=1).astype(jnp.bfloat16)
        rolled[l] = dot_nn(selector, whole).astype(jnp.bfloat16)

    tokens = 2 * cells
    level_k = lax.broadcasted_iota(jnp.int32, (tokens, tokens), 0) // cells
    level_q = lax.broadcasted_iota(jnp.int32, (tokens, tokens), 1) // cells
    allowed = jnp.where((level_k == level_q) | (wrapped == 0), 1.0, 0.0)

    def window(w, carry):
        at = pl.ds(pl.multiple_of(w * cells, cells), cells)
        block = jnp.concatenate([rolled[0, at, :], rolled[1, at, :]], axis=0)
        out = attend_window(block, allowed)
        result[0, at, :] = out[:cells]
        result[1, at, :] = out[cells:]
        return carry

    lax.fori_loop(0, tiles_count, window, 0)

    zero = jnp.zeros((plane, LANES), jnp.bfloat16)
    inner, outer = [], []
    for l in range(2):
        tok = dot_nn(back_selector, result[l]).astype(jnp.bfloat16)
        tail = tok[:, split + LANES :]
        inner.append(jnp.concatenate([tok[:, :split], zero, jnp.where(low, tail, zero)], axis=1))
        outer.append(jnp.concatenate([tok[:, split : split + LANES], jnp.where(low, zero, tail)], axis=1))
        grad_hidden = dot_nt(inner[l], wts[...]).astype(jnp.bfloat16)
        mixed_out = dot_nt(outer[l], wts[:, split:]).astype(jnp.bfloat16)
        for k in range(tiles_count):
            ref = send_ref if k % 2 else keep_ref
            at = slice(k * cells, (k + 1) * cells)
            ref[k // 2, l, :, :channels] = mixed_out[at]
            ref[k // 2, l, :, channels:] = grad_hidden[at]
    inner = jnp.concatenate(inner, axis=0)
    outer = jnp.concatenate(outer, axis=0)
    hid_t = hid[...].T
    up_t = up[...].T
    width = 3 * LANES
    share_b = dot_nn(hid_t, inner[:, width:])
    share_b = jnp.concatenate(
        [share_b[:, :LANES], share_b[:, LANES:] + dot_nn(up_t, outer)], axis=1
    ).astype(jnp.bfloat16)
    share_a = dot_nn(hid_t, inner[:, :width]).astype(jnp.bfloat16)
    half = rows // 2
    for share, keep, send in ((share_b, keep_b, send_b), (share_a, keep_a, send_a)):
        for j in range(tiles_count):
            first = share[j * rows : j * rows + half]
            second = share[j * rows + half : (j + 1) * rows]
            keep[j] = jnp.where(rep == 0, first, second)
            send[j] = jnp.where(rep == 0, second, first)


def column_kernel(here_ref, *refs):
    *slot_refs, out_ref = refs
    here = here_ref[0]
    own = LANES + LANES // 2
    channels = own * len(slot_refs)
    blocks = in_order([ref[...] for ref in slot_refs], here)
    pieces = []
    for which in range(2):
        for block in blocks:
            pieces.append(block[:, which * LANES : (which + 1) * LANES])
            rest = 2 * LANES + which * (LANES // 2)
            pieces.append(block[:, rest : rest + LANES // 2])
    out_ref[...] = jnp.concatenate(pieces, axis=1)


SMEM_SPEC = pl.BlockSpec(memory_space=pltpu.SMEM)
VMEM_SPEC = pl.BlockSpec(memory_space=pltpu.VMEM)


def call(body, outs, scalars, arrays, flops, name, scratch=()):
    moved = sum(a.size * a.dtype.itemsize for a in arrays) + sum(o.size * o.dtype.itemsize for o in outs)
    return pl.pallas_call(
        body,
        out_shape=outs,
        in_specs=[SMEM_SPEC] + [VMEM_SPEC] * len(arrays),
        out_specs=[VMEM_SPEC] * len(outs),
        scratch_shapes=list(scratch),
        compiler_params=pltpu.CompilerParams(vmem_limit_bytes=48 * 1024 * 1024),
        cost_estimate=pl.CostEstimate(flops=flops, bytes_accessed=moved, transcendentals=0),
        name=name,
    )(scalars, *arrays)


def low_shape(*shape):
    return jax.ShapeDtypeStruct(shape, jnp.bfloat16)


def added(a, b):
    return (a.astype(jnp.float32) + b.astype(jnp.float32)).astype(jnp.bfloat16)


def parted(value, dim, bit):
    size = value.shape[dim] // 2
    keep = lax.dynamic_slice_in_dim(value, bit * size, size, dim)
    send = lax.dynamic_slice_in_dim(value, (1 - bit) * size, size, dim)
    return keep, send


def joined(mine, other, bit, dim=0):
    odd = bit == 1
    return jnp.concatenate([jnp.where(odd, other, mine), jnp.where(odd, mine, other)], axis=dim)


def bits_of(count):
    bits, bit = [], 1
    while bit < count:
        bits.append(bit)
        bit *= 2
    return bits


def reduce_share(keep, send, lev_here, tile_here):
    part = added(keep, swapped(send, "rep", 1))
    levs = lax.axis_size("lev")
    for bit in bits_of(levs):
        keep, send = parted(part, 1, (lev_here // bit) % 2)
        part = added(keep, swapped(send, "lev", bit))
    tiles_count = lax.axis_size("tile")
    near = tile_here % 2
    pairs = part.reshape(tiles_count // 2, 2, *part.shape[1:])
    mine = lax.dynamic_index_in_dim(pairs, near, 1, keepdims=False)
    away = lax.dynamic_index_in_dim(pairs, 1 - near, 1, keepdims=False)
    came = swapped(away, "tile", 1)
    both = jnp.stack([mine, came], axis=1)
    far = tile_here // 2
    slots = lax.dynamic_index_in_dim(both, far, 0, keepdims=False)
    found = [slots[0], slots[1]]
    for mask in range(1, tiles_count // 2):
        got = swapped(lax.dynamic_index_in_dim(both, far ^ mask, 0, keepdims=False), "tile", 2 * mask)
        found += [got[0], got[1]]
    rows, cols = part.shape[1:]
    channels = tiles_count * cols // 2
    return call(
        column_kernel, [low_shape(rows, 2 * channels)], tile_here.reshape(1).astype(jnp.int32), found, 1000, "columns"
    )[0]


def spread(piece, lev_here, rep_here):
    for bit in reversed(bits_of(lax.axis_size("lev"))):
        piece = joined(piece, swapped(piece, "lev", bit), (lev_here // bit) % 2)
    return joined(piece, swapped(piece, "rep", 1), rep_here)


def shards_by_heads(tokens, w_qkv, w_proj, seam_codes, upstream):
    levels, extent, channels = tokens.shape[1], tokens.shape[3], tokens.shape[5]
    cells = extent * extent
    tiles_count = lax.axis_size("tile")
    rep_here, lev_here, tile_here = lax.axis_index("rep"), lax.axis_index("lev"), lax.axis_index("tile")
    shard_rows = w_qkv.shape[0]
    wrapped = lev_here == lax.axis_size("lev") - 1
    field_in = tokens.reshape(levels, cells, channels)
    field_up = upstream.reshape(levels, cells, channels)
    here = tile_here.reshape(1).astype(jnp.int32)

    both = jnp.concatenate([field_in, field_up], axis=-1)
    high, low = both[1], shifted(both[0], "lev", -1)
    blocks = call(
        deal_kernel, [low_shape(shard_rows, channels)] * tiles_count, here, [w_qkv, w_proj], 1000, "deal"
    )
    blocks = [blocks[0]] + [swapped(blocks[k], "tile", k) for k in range(1, tiles_count)]

    def gathered(piece):
        have = {0: piece}
        for bit in reversed(bits_of(tiles_count)):
            for k in list(have):
                have[k ^ bit] = swapped(have[k], "tile", bit)
        return [have[k] for k in range(tiles_count)]

    pieces = [p for pair in zip(gathered(high), gathered(low)) for p in pair]
    source = roll_source(seam_codes, tile_here, tiles_count, extent)
    scalars = jnp.stack([wrapped.astype(jnp.int32), rep_here.astype(jnp.int32), tile_here.astype(jnp.int32)])
    plane = tiles_count * cells
    half = shard_rows // 2
    width = 3 * LANES
    sums_shape = low_shape(tiles_count // 2, levels, cells, 2 * channels)
    part_shape = low_shape(tiles_count, half, width)
    keep, send, keep_a, send_a, keep_b, send_b = call(
        main_kernel,
        [sums_shape, sums_shape, part_shape, part_shape, part_shape, part_shape],
        scalars,
        [source.reshape(-1, 1), source.reshape(1, -1), *pieces, *blocks],
        8 * levels * plane * channels * channels,
        "main",
        scratch=[
            pltpu.VMEM((levels * plane, channels), jnp.bfloat16),
            pltpu.VMEM((levels * plane, channels), jnp.bfloat16),
            pltpu.VMEM((channels, 2 * width), jnp.bfloat16),
            pltpu.VMEM((levels, plane, 2 * width), jnp.bfloat16),
            pltpu.VMEM((levels, plane, 2 * width), jnp.bfloat16),
        ],
    )

    sums = added(keep, swapped(send, "tile", 1))
    slots = [sums[k] for k in range(tiles_count // 2)]
    for bit in bits_of(tiles_count // 2):
        came = swapped(jnp.stack(slots[1::2]), "tile", 2 * bit)
        slots = [added(slots[2 * k], came[k]) for k in range(len(slots) // 2)]
    final = slots[0]
    low_back = shifted(final[1], "lev", 1)
    final = jnp.stack([low_back, final[0]]).reshape(levels * cells, 2 * channels)
    token_rows = field_in.reshape(-1, channels)
    upstream_rows = field_up.reshape(-1, channels)
    normalized, inverse = layer_stats(token_rows)
    output = (token_rows.astype(jnp.float32) + final[:, :channels].astype(jnp.float32)).astype(jnp.bfloat16)
    grad_tokens = norm_backward(upstream_rows, final[:, channels:].astype(jnp.float32), normalized, inverse)

    grad_b, grad_a = [
        spread(reduce_share(*pair, lev_here, tile_here), lev_here, rep_here).astype(jnp.float32)
        for pair in ((keep_b, send_b), (keep_a, send_a))
    ]
    grad_qkv = jnp.concatenate([grad_a, grad_b[:, :channels]], axis=1)
    grad_proj = grad_b[:, channels:]
    return (output.reshape(tokens.shape), grad_tokens.reshape(tokens.shape), grad_qkv, grad_proj)


def power_of_two(count):
    return count & (count - 1) == 0


def shards(tokens, w_qkv, w_proj, seam_codes, upstream):
    counts = [lax.axis_size(axis) for axis in ("rep", "lev", "tile")]
    tiles_count = counts[2]
    channels = tokens.shape[5]
    one_window = tokens.shape[0] == 1 and tokens.shape[1] == WIN_LEV and tokens.shape[3] == WIN and tokens.shape[2] == 1
    by_heads = (
        one_window
        and all(power_of_two(count) for count in counts)
        and tiles_count % 4 == 0
        and (channels // HEAD_DIM) % tiles_count == 0
        and channels // tiles_count == LANES + LANES // 2
        and counts[0] == 2
        and (channels // tiles_count) % (8 * counts[0] * counts[1]) == 0
    )
    body = shards_by_heads if by_heads else shards_general
    return body(tokens, w_qkv, w_proj, seam_codes, upstream)


def solution(mesh):
    in_specs = (
        P("rep", "lev", "tile", None, None, None),
        P("tile", None),
        P("tile", None),
        P(),
        P("rep", "lev", "tile", None, None, None),
    )
    out_specs = (
        P("rep", "lev", "tile", None, None, None),
        P("rep", "lev", "tile", None, None, None),
        P("tile", None),
        P("tile", None),
    )
    return jax.shard_map(shards, mesh=mesh, in_specs=in_specs, out_specs=out_specs, check_vma=False)
```

```python
import jax
import jax.numpy as jnp
from jax import lax
from jax.experimental import pallas as pl
from jax.experimental.pallas import tpu as pltpu
from jax.sharding import PartitionSpec as P

HEAD_DIM = 32
WIN = 8
WIN_LEV = 2


EPSILON = 1e-05


def shifted(value, axis, steps):
    count = lax.axis_size(axis)
    pairs = [(source, (source + steps) % count) for source in range(count)]
    return lax.ppermute(value, axis, pairs)


def layer_stats(token_rows):
    values = token_rows.astype(jnp.float32)
    center = jnp.mean(values, axis=1, keepdims=True)
    spread = jnp.mean(jnp.square(values - center), axis=1, keepdims=True)
    inverse = lax.rsqrt(spread + EPSILON)
    return ((values - center) * inverse, inverse)


def norm_backward(upstream_rows, grad_hidden, normalized, inverse):
    centre = jnp.mean(grad_hidden, axis=1, keepdims=True)
    projected = jnp.mean(grad_hidden * normalized, axis=1, keepdims=True)
    total_grad = (
        upstream_rows.astype(jnp.float32)
        + (grad_hidden - centre - normalized * projected) * inverse
    )
    return total_grad.astype(jnp.bfloat16)


def roll_local(grid_field, east_flag, north_flag, north_step):
    shift_cells = WIN // 2
    east_part = shifted(grid_field[:, :, :shift_cells], "tile", -1)
    east_part = jnp.where(east_flag, east_part[:, ::-1], east_part)
    across = jnp.concatenate([grid_field[:, :, shift_cells:], east_part], axis=2)
    north_part = shifted(across[:, :shift_cells], "tile", -north_step)
    north_part = jnp.where(north_flag, north_part[:, :, ::-1], north_part)
    upward = jnp.concatenate([across[:, shift_cells:], north_part], axis=1)
    level_part = shifted(upward[:1], "lev", -1)
    return jnp.concatenate([upward[1:], level_part], axis=0)


def unroll_local(rolled, east_flag, north_flag, north_step):
    shift_cells = WIN // 2
    extent = rolled.shape[1]
    level_part = shifted(rolled[-1:], "lev", 1)
    upward = jnp.concatenate([level_part, rolled[:-1]], axis=0)
    north_part = upward[:, extent - shift_cells :]
    north_part = jnp.where(north_flag, north_part[:, :, ::-1], north_part)
    north_part = shifted(north_part, "tile", north_step)
    across = jnp.concatenate([north_part, upward[:, : extent - shift_cells]], axis=1)
    east_part = across[:, :, extent - shift_cells :]
    east_part = jnp.where(east_flag, east_part[:, ::-1], east_part)
    east_part = shifted(east_part, "tile", 1)
    return jnp.concatenate([east_part, across[:, :, : extent - shift_cells]], axis=2)


def to_windows(grid_field):
    levels = grid_field.shape[0]
    extent = grid_field.shape[1]
    channels = grid_field.shape[3]
    blocks = grid_field.reshape(
        levels // WIN_LEV, WIN_LEV, extent // WIN, WIN, extent // WIN, WIN, channels
    )
    blocks = blocks.transpose(0, 2, 4, 1, 3, 5, 6)
    return blocks.reshape(-1, WIN_LEV * WIN * WIN, channels)


def from_windows(windows, levels, extent):
    channels = windows.shape[-1]
    blocks = windows.reshape(
        levels // WIN_LEV, extent // WIN, extent // WIN, WIN_LEV, WIN, WIN, channels
    )
    blocks = blocks.transpose(0, 3, 1, 4, 2, 5, 6)
    return blocks.reshape(levels, extent, extent, channels)


def split_heads(packed):
    windows = packed.shape[0]
    tokens = packed.shape[1]
    model_width = packed.shape[2] // 3
    head_count = model_width // HEAD_DIM
    query_part = packed[:, :, :model_width].reshape(windows, tokens, head_count, HEAD_DIM)
    key_part = packed[:, :, model_width : 2 * model_width].reshape(
        windows, tokens, head_count, HEAD_DIM
    )
    value_part = packed[:, :, 2 * model_width :].reshape(windows, tokens, head_count, HEAD_DIM)
    return (query_part, key_part, value_part)


def window_mask(wrap_flags, tokens):
    level_of = jnp.arange(tokens, dtype=jnp.int32) // (WIN * WIN)
    same_level = level_of[:, None] == level_of[None, :]
    allowed = jnp.logical_or(
        same_level[None, None], jnp.logical_not(wrap_flags)[:, None, None, None]
    )
    return allowed.astype(jnp.float32)


def attend_forward(packed, wrap_flags):
    query_part, key_part, value_part = split_heads(packed)
    scores = jnp.einsum(
        "wqhd,wkhd->whqk", query_part, key_part, preferred_element_type=jnp.float32
    ) * HEAD_DIM ** (-0.5)
    raised = jnp.exp(scores) * window_mask(wrap_flags, packed.shape[1])
    prob = raised / jnp.sum(raised, axis=-1, keepdims=True)
    prob_low = prob.astype(jnp.bfloat16)
    attended = jnp.einsum(
        "whqk,wkhd->wqhd", prob_low, value_part, preferred_element_type=jnp.float32
    )
    attended = attended.astype(jnp.bfloat16).reshape(packed.shape[0], packed.shape[1], -1)
    return (attended, prob, prob_low)


def attend_backward(packed, back_windows, prob, prob_low):
    query_part, key_part, value_part = split_heads(packed)
    back_heads = back_windows.reshape(query_part.shape)
    grad_value = jnp.einsum(
        "whqk,wqhd->wkhd", prob_low, back_heads, preferred_element_type=jnp.float32
    )
    grad_prob = jnp.einsum(
        "wqhd,wkhd->whqk", back_heads, value_part, preferred_element_type=jnp.float32
    )
    centre = jnp.sum(prob * grad_prob, axis=-1, keepdims=True)
    grad_scores = (prob * (grad_prob - centre) * HEAD_DIM ** (-0.5)).astype(jnp.bfloat16)
    grad_query = jnp.einsum(
        "whqk,wkhd->wqhd", grad_scores, key_part, preferred_element_type=jnp.float32
    )
    grad_key = jnp.einsum(
        "whqk,wqhd->wkhd", grad_scores, query_part, preferred_element_type=jnp.float32
    )
    windows = packed.shape[0]
    tokens = packed.shape[1]
    joined = jnp.concatenate(
        [
            grad_query.reshape(windows, tokens, -1),
            grad_key.reshape(windows, tokens, -1),
            grad_value.reshape(windows, tokens, -1),
        ],
        axis=-1,
    )
    return joined.astype(jnp.bfloat16)


def shards_general(tokens, w_qkv, w_proj, seam_codes, upstream):
    levels = tokens.shape[1]
    extent = tokens.shape[3]
    model_width = tokens.shape[5]
    tiles_count = lax.axis_size("tile")
    north_step = tiles_count // 4
    tile_here = lax.axis_index("tile")
    east_flag = seam_codes[tile_here, 0] == 1
    north_flag = seam_codes[tile_here, 1] == 1
    top_level = lax.axis_index("lev") == lax.axis_size("lev") - 1
    per_level = extent // WIN * (extent // WIN)
    window_total = levels // WIN_LEV * per_level
    lev_window = jnp.arange(window_total, dtype=jnp.int32) // per_level
    wrap_flags = jnp.logical_and(top_level, lev_window == levels // WIN_LEV - 1)
    contract_last = (((1,), (1,)), ((), ()))
    contract_first = (((0,), (0,)), ((), ()))
    grid_in = tokens.reshape(levels, extent, extent, model_width)
    grid_up = upstream.reshape(levels, extent, extent, model_width)
    paired = roll_local(
        jnp.concatenate([grid_in, grid_up], axis=-1), east_flag, north_flag, north_step
    )
    grid_in = paired[..., :model_width]
    grid_up = paired[..., model_width:]
    token_rows = grid_in.reshape(-1, model_width)
    upstream_rows = grid_up.reshape(-1, model_width)
    normalized, inverse = layer_stats(token_rows)
    hidden = normalized.astype(jnp.bfloat16)
    full_qkv, full_proj = (
        lax.all_gather(w_qkv, "tile", axis=0, tiled=True),
        lax.all_gather(w_proj, "tile", axis=0, tiled=True),
    )
    projected = jnp.dot(hidden, full_qkv, preferred_element_type=jnp.float32).astype(jnp.bfloat16)
    grid_qkv = projected.reshape(levels, extent, extent, 3 * model_width)
    windows_qkv = to_windows(grid_qkv)
    attended, prob, prob_low = attend_forward(windows_qkv, wrap_flags)
    grid_mixed = from_windows(attended, levels, extent)
    mixed_in = grid_mixed.reshape(-1, model_width)
    mixed_out = lax.dot_general(
        mixed_in, full_proj, contract_last, preferred_element_type=jnp.float32
    )
    back_mix = jnp.dot(upstream_rows, full_proj, preferred_element_type=jnp.float32)
    output_low = (token_rows.astype(jnp.float32) + mixed_out).astype(jnp.bfloat16)
    back_low = back_mix.astype(jnp.bfloat16)
    grid_back = back_low.reshape(levels, extent, extent, model_width)
    grad_windows = attend_backward(windows_qkv, to_windows(grid_back), prob, prob_low)
    grid_grad = from_windows(grad_windows, levels, extent)
    grad_qkv_tok = grid_grad.reshape(-1, 3 * model_width)
    grad_hidden = lax.dot_general(
        grad_qkv_tok, full_qkv, contract_last, preferred_element_type=jnp.float32
    )
    grad_low = norm_backward(upstream_rows, grad_hidden, normalized, inverse)
    grid_output = output_low.reshape(levels, extent, extent, model_width)
    grid_dx = grad_low.reshape(levels, extent, extent, model_width)
    paired = unroll_local(
        jnp.concatenate([grid_output, grid_dx], axis=-1), east_flag, north_flag, north_step
    )
    grid_output = paired[..., :model_width]
    grid_dx = paired[..., model_width:]
    columns = hidden
    share_qkv = lax.psum_scatter(
        lax.dot_general(
            columns, grad_qkv_tok, contract_first, preferred_element_type=jnp.float32
        ).astype(jnp.bfloat16),
        "tile",
        scatter_dimension=0,
        tiled=True,
    )
    columns = upstream_rows
    share_proj = lax.psum_scatter(
        lax.dot_general(
            columns, mixed_in, contract_first, preferred_element_type=jnp.float32
        ).astype(jnp.bfloat16),
        "tile",
        scatter_dimension=0,
        tiled=True,
    )
    grad_qkv, grad_proj = (
        lax.psum(share_qkv, ("rep", "lev")).astype(jnp.float32),
        lax.psum(share_proj, ("rep", "lev")).astype(jnp.float32),
    )
    return (grid_output.reshape(tokens.shape), grid_dx.reshape(tokens.shape), grad_qkv, grad_proj)


LANES = 128
MAIN_MEBIBYTES = 56
NEAR = LANES // HEAD_DIM


def swapped(value, axis, mask):
    count = lax.axis_size(axis)
    return lax.ppermute(value, axis, [(source, source ^ mask) for source in range(count)])


def roll_source(codes_ref, cell, tile_here, tiles_count, extent):
    half = WIN // 2
    north_step = tiles_count // 4
    slot = cell // (extent * extent)
    row = (cell // extent) % extent
    col = cell % extent

    def code_of(tile, which):
        found = jnp.zeros_like(tile)
        for t in range(tiles_count):
            found = jnp.where(tile == t, codes_ref[t, which], found)
        return found == 1

    tile = jnp.bitwise_xor(slot, tile_here)
    crossed = row >= extent - half
    col1 = jnp.where(crossed & code_of(tile, 1), extent - 1 - col, col)
    row1 = jnp.where(crossed, row - (extent - half), row + half)
    tile1 = jnp.where(crossed, (tile + north_step) % tiles_count, tile)
    crossed = col1 >= extent - half
    row2 = jnp.where(crossed & code_of(tile1, 0), extent - 1 - row1, row1)
    col2 = jnp.where(crossed, col1 - (extent - half), col1 + half)
    tile2 = jnp.where(crossed, (tile1 + 1) % tiles_count, tile1)
    return (jnp.bitwise_xor(tile2, tile_here) * extent + row2) * extent + col2


def in_order(slots, here):
    bit = 1
    while bit < len(slots):
        odd = jnp.bitwise_and(here, bit) != 0
        slots = [jnp.where(odd, slots[k ^ bit], slots[k]) for k in range(len(slots))]
        bit *= 2
    return slots


def dot_nn(a, b):
    return lax.dot_general(a, b, (((1,), (0,)), ((), ())), preferred_element_type=jnp.float32)


def dot_nt(a, b):
    return lax.dot_general(a, b, (((1,), (1,)), ((), ())), preferred_element_type=jnp.float32)


def dot_tn(a, b):
    return lax.dot_general(a, b, (((0,), (0,)), ((), ())), preferred_element_type=jnp.float32)


def deal_kernel(scal_ref, qkv_any, out_any, in_any, up_any, high_ref, low_ref, *refs):
    *block_refs, qkv_ref, out_ref, sems = refs
    tiles_count = len(block_refs)
    channels = out_ref.shape[1]
    own = channels // tiles_count
    rep, here = scal_ref[0], scal_ref[1]
    copies = [
        pltpu.make_async_copy(source.at[level], target.at[:, first : first + channels], sems.at[2 * level + which])
        for level, target in ((0, low_ref), (1, high_ref))
        for which, (source, first) in enumerate(((in_any, 0), (up_any, channels)))
    ]
    copies.append(pltpu.make_async_copy(qkv_any, qkv_ref, sems.at[4]))
    copies.append(pltpu.make_async_copy(out_any, out_ref, sems.at[5]))
    for copy in copies:
        copy.start()
    for copy in copies:
        copy.wait()

    def columns(which, tile):
        ref = out_ref if which == 3 else qkv_ref
        base = (0 if which == 3 else which * channels) + tile * own
        return ref[:, base : base + LANES], ref[:, base + LANES : base + own]

    blocks = []
    for tile in range(tiles_count):
        (q, q1), (k, k1), (v, v1), (p, p1) = [columns(which, tile) for which in range(4)]
        blocks.append(jnp.concatenate([q, k, q1, k1, v, p, v1, p1], axis=1))
    for slot, (ref, block) in enumerate(zip(block_refs, in_order(blocks, here))):
        if slot >= 2:
            half = block.shape[0] // 2
            block = jnp.where(rep == 0, block[:half], block[half:])
        ref[...] = block


def attend_window(block, allowed):
    tokens = block.shape[0]
    lane = lax.broadcasted_iota(jnp.int32, (1, LANES), 1)
    group = [block[:, g * LANES : (g + 1) * LANES] for g in range(6)]
    scale = HEAD_DIM ** (-0.5)

    def turned(x):
        return pltpu.roll(x.astype(jnp.float32), LANES // 2, 1)

    def attend(q, k, v, o, heads):
        masks = [lane // HEAD_DIM == h for h in range(heads)]

        def stacked(x):
            return jnp.concatenate([jnp.where(m, x, jnp.zeros_like(x)) for m in masks], axis=0)

        def folded(x):
            total = jnp.where(masks[0], x[:tokens], 0.0)
            for h in range(1, heads):
                total = jnp.where(masks[h], x[h * tokens : (h + 1) * tokens], total)
            return total

        k_all, v_all = stacked(k), stacked(v)
        scores = (dot_nt(k_all, q) * scale).reshape(heads, tokens, tokens)
        raised = jnp.exp(scores) * allowed[None]
        prob = raised / jnp.sum(raised, axis=1, keepdims=True)
        grad_prob = dot_nt(v_all, o).reshape(heads, tokens, tokens)
        centre = jnp.sum(prob * grad_prob, axis=1, keepdims=True)
        grad_scores = (prob * (grad_prob - centre) * scale).astype(jnp.bfloat16).reshape(-1, tokens)
        prob_low = prob.astype(jnp.bfloat16).reshape(-1, tokens)
        att = dot_tn(prob_low, v_all)
        grad_q = dot_tn(grad_scores, k_all)
        grad_k = folded(dot_nn(grad_scores, q))
        grad_v = folded(dot_nn(prob_low, o))
        return grad_q, grad_k, grad_v, att

    gq, gk, gv, att = attend(group[0], group[1], group[3], group[4], NEAR)
    qk_turned = turned(group[2]).astype(jnp.bfloat16)
    vo_turned = turned(group[5]).astype(jnp.bfloat16)
    gq1, gk1, gv1, att1 = attend(group[2], qk_turned, group[5], vo_turned, NEAR // 2)
    parts = [gq, gk, gq1 + turned(gk1), gv, att, gv1 + turned(att1)]
    return jnp.concatenate(parts, axis=1).astype(jnp.bfloat16)


def main_kernel(scal_ref, codes_ref, *refs):
    *refs, inner_ref, outer_ref, wts, keep_a, send_a, keep_b, send_b, hid, up, rolled, result, fields, sems = refs
    tiles_count = (len(refs) + 2) // 4
    cells_refs = refs[: 2 * tiles_count]
    near_refs = refs[2 * tiles_count : 2 * tiles_count + 2]
    far_refs = refs[2 * tiles_count + 2 :]
    cells = cells_refs[0].shape[0]
    channels = wts.shape[0]
    rows = channels // tiles_count
    half = rows // 2
    plane = tiles_count * cells
    wrapped, rep, here = scal_ref[0], scal_ref[1], scal_ref[2]
    copies = []

    def fetch(source, target):
        copy = pltpu.make_async_copy(source, target, sems.at[len(copies)])
        copy.start()
        copies.append(copy)

    for k in range(tiles_count):
        for l in range(2):
            fetch(cells_refs[2 * k + l], fields.at[pl.ds(l * plane + k * cells, cells)])
    for k in range(tiles_count):
        base = (here ^ k) * rows
        if k < 2:
            fetch(near_refs[k], wts.at[pl.ds(pl.multiple_of(base, 32), rows)])
        else:
            fetch(far_refs[2 * k - 4], wts.at[pl.ds(pl.multiple_of(base + rep * half, 32), half)])
            fetch(far_refs[2 * k - 3], wts.at[pl.ds(pl.multiple_of(base + (1 - rep) * half, 32), half)])
    for copy in copies[: 2 * tiles_count]:
        copy.wait()
    for at in range(0, 2 * plane, cells):
        x = fields[at : at + cells, :channels].astype(jnp.float32)
        center = jnp.mean(x, axis=1, keepdims=True)
        x = x - center
        spread = jnp.mean(jnp.square(x), axis=1, keepdims=True)
        hid[at : at + cells, :] = (x * lax.rsqrt(spread + EPSILON)).astype(jnp.bfloat16)
        up[at : at + cells, :] = fields[at : at + cells, channels:]
    for copy in copies[2 * tiles_count :]:
        copy.wait()

    lane = lax.broadcasted_iota(jnp.int32, (1, LANES), 1)
    low = lane < LANES // 2
    split = 4 * LANES
    extent = WIN
    source = roll_source(codes_ref, lax.broadcasted_iota(jnp.int32, (plane, 1), 0), here, tiles_count, extent)
    from_col = lax.broadcasted_iota(jnp.int32, (plane, plane), 1) == source
    selector = jnp.where(from_col, 1.0, 0.0).astype(jnp.bfloat16)
    source = roll_source(codes_ref, lax.broadcasted_iota(jnp.int32, (1, plane), 1), here, tiles_count, extent)
    from_row = lax.broadcasted_iota(jnp.int32, (plane, plane), 0) == source
    back_selector = jnp.where(from_row, 1.0, 0.0).astype(jnp.bfloat16)
    for l in range(2):
        at = slice(l * plane, (l + 1) * plane)
        front = dot_nn(hid[at, :], wts[:, :split])
        last = dot_nn(hid[at, :], wts[:, split + LANES :])
        back = dot_nn(up[at, :], wts[:, split:])
        mixed = jnp.where(low, last, back[:, LANES:])
        whole = jnp.concatenate([front, back[:, :LANES], mixed], axis=1).astype(jnp.bfloat16)
        rolled[l] = dot_nn(selector, whole).astype(jnp.bfloat16)

    tokens = 2 * cells
    level_k = lax.broadcasted_iota(jnp.int32, (tokens, tokens), 0) // cells
    level_q = lax.broadcasted_iota(jnp.int32, (tokens, tokens), 1) // cells
    allowed = jnp.where((level_k == level_q) | (wrapped == 0), 1.0, 0.0)

    def window(w, carry):
        at = pl.ds(pl.multiple_of(w * cells, cells), cells)
        block = jnp.concatenate([rolled[0, at, :], rolled[1, at, :]], axis=0)
        out = attend_window(block, allowed)
        result[0, at, :] = out[:cells]
        result[1, at, :] = out[cells:]
        return carry

    lax.fori_loop(0, tiles_count, window, 0)

    zero = jnp.zeros((plane, LANES), jnp.bfloat16)
    for l in range(2):
        at = slice(l * plane, (l + 1) * plane)
        tok = dot_nn(back_selector, result[l]).astype(jnp.bfloat16)
        tail = tok[:, split + LANES :]
        inner_ref[at, :] = jnp.concatenate([tok[:, :split], zero, jnp.where(low, tail, zero)], axis=1)
        outer_ref[at, :] = jnp.concatenate([tok[:, split : split + LANES], jnp.where(low, zero, tail)], axis=1)
    inner, outer = inner_ref[...], outer_ref[...]
    hid_t = hid[...].T
    up_t = up[...].T
    width = 3 * LANES
    share_b = dot_nn(hid_t, inner[:, width:])
    share_b = jnp.concatenate(
        [share_b[:, :LANES], share_b[:, LANES:] + dot_nn(up_t, outer)], axis=1
    ).astype(jnp.bfloat16)
    share_a = dot_nn(hid_t, inner[:, :width]).astype(jnp.bfloat16)
    for share, keep, send in ((share_b, keep_b, send_b), (share_a, keep_a, send_a)):
        for j in range(tiles_count):
            first = share[j * rows : j * rows + half]
            second = share[j * rows + half : (j + 1) * rows]
            keep[j] = jnp.where(rep == 0, first, second)
            send[j] = jnp.where(rep == 0, second, first)


def rows_kernel(inner_ref, outer_ref, wts, keep_ref, send_ref):
    slots, levels, cells, width = keep_ref.shape
    channels = width // 2
    plane = 2 * slots * cells
    split = 4 * LANES
    for l in range(levels):
        at = slice(l * plane, (l + 1) * plane)
        grad_hidden = dot_nt(inner_ref[at, :], wts[...]).astype(jnp.bfloat16)
        mixed_out = dot_nt(outer_ref[at, :], wts[:, split:]).astype(jnp.bfloat16)
        for k in range(2 * slots):
            ref = send_ref if k % 2 else keep_ref
            at = slice(k * cells, (k + 1) * cells)
            ref[k // 2, l, :, :channels] = mixed_out[at]
            ref[k // 2, l, :, channels:] = grad_hidden[at]


def column_kernel(here_ref, *refs):
    *slot_refs, out_ref = refs
    here = here_ref[0]
    blocks = in_order([ref[...] for ref in slot_refs], here)
    pieces = []
    for which in range(2):
        for block in blocks:
            pieces.append(block[:, which * LANES : (which + 1) * LANES])
            rest = 2 * LANES + which * (LANES // 2)
            pieces.append(block[:, rest : rest + LANES // 2])
    out_ref[...] = jnp.concatenate(pieces, axis=1)


SMEM_SPEC = pl.BlockSpec(memory_space=pltpu.SMEM)
VMEM_SPEC = pl.BlockSpec(memory_space=pltpu.VMEM)
ANY_SPEC = pl.BlockSpec(memory_space=pl.ANY)


def call(body, outs, scalars, arrays, flops, mebibytes, scratch=(), spec=VMEM_SPEC):
    moved = sum(a.size * a.dtype.itemsize for a in arrays) + sum(o.size * o.dtype.itemsize for o in outs)
    return pl.pallas_call(
        body,
        out_shape=outs,
        in_specs=[SMEM_SPEC] * len(scalars) + [spec] * len(arrays),
        out_specs=[VMEM_SPEC] * len(outs),
        scratch_shapes=list(scratch),
        compiler_params=pltpu.CompilerParams(vmem_limit_bytes=mebibytes * 1024 * 1024),
        cost_estimate=pl.CostEstimate(flops=flops, bytes_accessed=moved, transcendentals=0),
    )(*scalars, *arrays)


def low_shape(*shape):
    return jax.ShapeDtypeStruct(shape, jnp.bfloat16)


def added(a, b):
    return (a.astype(jnp.float32) + b.astype(jnp.float32)).astype(jnp.bfloat16)


def parted(value, dim, bit):
    size = value.shape[dim] // 2
    keep = lax.dynamic_slice_in_dim(value, bit * size, size, dim)
    send = lax.dynamic_slice_in_dim(value, (1 - bit) * size, size, dim)
    return keep, send


def joined(mine, other, bit, dim=0):
    odd = bit == 1
    return jnp.concatenate([jnp.where(odd, other, mine), jnp.where(odd, mine, other)], axis=dim)


def bits_of(count):
    bits, bit = [], 1
    while bit < count:
        bits.append(bit)
        bit *= 2
    return bits


def reduce_share(keep, send, lev_here, tile_here):
    came = swapped(send, "rep", 1)
    part = added(keep, came)
    for bit in bits_of(lax.axis_size("lev")):
        keep, send = parted(part, 1, (lev_here // bit) % 2)
        came = swapped(send, "lev", bit)
        part = added(keep, came)
    tiles_count = lax.axis_size("tile")
    near = tile_here % 2
    pairs = part.reshape(tiles_count // 2, 2, *part.shape[1:])
    mine = lax.dynamic_index_in_dim(pairs, near, 1, keepdims=False)
    away = lax.dynamic_index_in_dim(pairs, 1 - near, 1, keepdims=False)
    came = swapped(away, "tile", 1)
    both = jnp.stack([mine, came], axis=1)
    far = tile_here // 2
    slots = lax.dynamic_index_in_dim(both, far, 0, keepdims=False)
    found = [slots[0], slots[1]]
    for mask in range(1, tiles_count // 2):
        got = swapped(lax.dynamic_index_in_dim(both, far ^ mask, 0, keepdims=False), "tile", 2 * mask)
        found += [got[0], got[1]]
    rows, cols = part.shape[1:]
    channels = tiles_count * cols // 2
    here = tile_here.reshape(1).astype(jnp.int32)
    return call(column_kernel, [low_shape(rows, 2 * channels)], [here], found, 1000, 4)[0]


def spread(piece, lev_here, rep_here):
    for bit in reversed(bits_of(lax.axis_size("lev"))):
        came = swapped(piece, "lev", bit)
        piece = joined(piece, came, (lev_here // bit) % 2)
    came = swapped(piece, "rep", 1)
    return joined(piece, came, rep_here)


def shards_by_heads(tokens, w_qkv, w_proj, seam_codes, upstream):
    levels, extent, channels = tokens.shape[1], tokens.shape[3], tokens.shape[5]
    cells = extent * extent
    tiles_count = lax.axis_size("tile")
    rep_here, lev_here, tile_here = lax.axis_index("rep"), lax.axis_index("lev"), lax.axis_index("tile")
    shard_rows = w_qkv.shape[0]
    wrapped = lev_here == lax.axis_size("lev") - 1
    field_in = tokens.reshape(levels, cells, channels)
    field_up = upstream.reshape(levels, cells, channels)
    half = shard_rows // 2

    shape = low_shape(cells, 2 * channels)
    high, low, *blocks = call(
        deal_kernel,
        [shape, shape]
        + [low_shape(shard_rows, channels)] * 2
        + [low_shape(half, channels)] * (tiles_count - 2),
        [jnp.stack([rep_here.astype(jnp.int32), tile_here.astype(jnp.int32)])],
        [w_qkv, w_proj, field_in, field_up],
        1000,
        MAIN_MEBIBYTES,
        scratch=[
            pltpu.VMEM(w_qkv.shape, jnp.bfloat16),
            pltpu.VMEM(w_proj.shape, jnp.bfloat16),
            pltpu.SemaphoreType.DMA((6,)),
        ],
        spec=ANY_SPEC,
    )
    low = shifted(low, "lev", -1)
    weights = [blocks[0]]
    for k in range(1, tiles_count):
        weights.append(swapped(blocks[k], "tile", k))
        if k >= 2:
            weights.append(swapped(weights[-1], "rep", 1))

    def gathered(piece):
        have = {0: piece}
        for bit in reversed(bits_of(tiles_count)):
            for k in list(have):
                have[k ^ bit] = swapped(have[k], "tile", bit)
        return [have[k] for k in range(tiles_count)]

    pieces = [p for pair in zip(gathered(high), gathered(low)) for p in pair]
    scalars = jnp.stack([wrapped.astype(jnp.int32), rep_here.astype(jnp.int32), tile_here.astype(jnp.int32)])
    plane = tiles_count * cells
    width = 3 * LANES
    part_shape = low_shape(tiles_count, half, width)
    inner_shape = low_shape(levels * plane, 2 * width)
    outer_shape = low_shape(levels * plane, 2 * LANES)
    weight_shape = low_shape(channels, 2 * width)
    inner, outer, weight, keep_a, send_a, keep_b, send_b = call(
        main_kernel,
        [inner_shape, outer_shape, weight_shape, part_shape, part_shape, part_shape, part_shape],
        [scalars, seam_codes],
        [*pieces, *weights],
        8 * levels * plane * channels * channels,
        MAIN_MEBIBYTES,
        scratch=[
            pltpu.VMEM((levels * plane, channels), jnp.bfloat16),
            pltpu.VMEM((levels * plane, channels), jnp.bfloat16),
            pltpu.VMEM((levels, plane, 2 * width), jnp.bfloat16),
            pltpu.VMEM((levels, plane, 2 * width), jnp.bfloat16),
            pltpu.VMEM((levels * plane, 2 * channels), jnp.bfloat16),
            pltpu.SemaphoreType.DMA((len(pieces) + len(weights),)),
        ],
        spec=ANY_SPEC,
    )
    sums_shape = low_shape(tiles_count // 2, levels, cells, 2 * channels)
    keep, send = call(rows_kernel, [sums_shape, sums_shape], [], [inner, outer, weight], 10**9, 16)

    came = swapped(send, "tile", 1)
    sums = added(keep, came)
    slots = [sums[k] for k in range(tiles_count // 2)]
    for bit in bits_of(tiles_count // 2):
        came = swapped(jnp.stack(slots[1::2]), "tile", 2 * bit)
        slots = [added(slots[2 * k], came[k]) for k in range(len(slots) // 2)]
    final = slots[0]
    low_back = shifted(final[1], "lev", 1)
    final = jnp.stack([low_back, final[0]]).reshape(levels * cells, 2 * channels)
    token_rows = field_in.reshape(-1, channels)
    upstream_rows = field_up.reshape(-1, channels)
    normalized, inverse = layer_stats(token_rows)
    output = (token_rows.astype(jnp.float32) + final[:, :channels].astype(jnp.float32)).astype(jnp.bfloat16)
    grad_tokens = norm_backward(upstream_rows, final[:, channels:].astype(jnp.float32), normalized, inverse)

    grad_b, grad_a = [
        spread(reduce_share(*pair, lev_here, tile_here), lev_here, rep_here).astype(jnp.float32)
        for pair in ((keep_b, send_b), (keep_a, send_a))
    ]
    grad_qkv = jnp.concatenate([grad_a, grad_b[:, :channels]], axis=1)
    grad_proj = grad_b[:, channels:]
    return (output.reshape(tokens.shape), grad_tokens.reshape(tokens.shape), grad_qkv, grad_proj)


def power_of_two(count):
    return count & (count - 1) == 0


def shards(tokens, w_qkv, w_proj, seam_codes, upstream):
    counts = [lax.axis_size(axis) for axis in ("rep", "lev", "tile")]
    tiles_count = counts[2]
    channels = tokens.shape[5]
    one_window = tokens.shape[0] == 1 and tokens.shape[1] == WIN_LEV and tokens.shape[3] == WIN and tokens.shape[2] == 1
    by_heads = (
        one_window
        and all(power_of_two(count) for count in counts)
        and tiles_count % 4 == 0
        and (channels // HEAD_DIM) % tiles_count == 0
        and channels // tiles_count == LANES + LANES // 2
        and counts[0] == 2
        and (channels // tiles_count) % (8 * counts[0] * counts[1]) == 0
    )
    if not by_heads:
        return shards_general(tokens, w_qkv, w_proj, seam_codes, upstream)
    return shards_by_heads(tokens, w_qkv, w_proj, seam_codes, upstream)


def solution(mesh):
    in_specs = (
        P("rep", "lev", "tile", None, None, None),
        P("tile", None),
        P("tile", None),
        P(),
        P("rep", "lev", "tile", None, None, None),
    )
    out_specs = (
        P("rep", "lev", "tile", None, None, None),
        P("rep", "lev", "tile", None, None, None),
        P("tile", None),
        P("tile", None),
    )
    return jax.shard_map(shards, mesh=mesh, in_specs=in_specs, out_specs=out_specs, check_vma=False)
```

```python
import jax
import jax.numpy as jnp
from jax import lax
from jax.experimental import pallas as pl
from jax.experimental.pallas import tpu as pltpu
from jax.sharding import PartitionSpec as P

HEAD_DIM = 32
WIN = 8
WIN_LEV = 2


EPSILON = 1e-05


def shifted(value, axis, steps):
    count = lax.axis_size(axis)
    pairs = [(source, (source + steps) % count) for source in range(count)]
    return lax.ppermute(value, axis, pairs)


def layer_stats(token_rows):
    values = token_rows.astype(jnp.float32)
    center = jnp.mean(values, axis=1, keepdims=True)
    spread = jnp.mean(jnp.square(values - center), axis=1, keepdims=True)
    inverse = lax.rsqrt(spread + EPSILON)
    return ((values - center) * inverse, inverse)


def norm_backward(upstream_rows, grad_hidden, normalized, inverse):
    centre = jnp.mean(grad_hidden, axis=1, keepdims=True)
    projected = jnp.mean(grad_hidden * normalized, axis=1, keepdims=True)
    total_grad = (
        upstream_rows.astype(jnp.float32)
        + (grad_hidden - centre - normalized * projected) * inverse
    )
    return total_grad.astype(jnp.bfloat16)


def roll_local(grid_field, east_flag, north_flag, north_step):
    shift_cells = WIN // 2
    east_part = shifted(grid_field[:, :, :shift_cells], "tile", -1)
    east_part = jnp.where(east_flag, east_part[:, ::-1], east_part)
    across = jnp.concatenate([grid_field[:, :, shift_cells:], east_part], axis=2)
    north_part = shifted(across[:, :shift_cells], "tile", -north_step)
    north_part = jnp.where(north_flag, north_part[:, :, ::-1], north_part)
    upward = jnp.concatenate([across[:, shift_cells:], north_part], axis=1)
    level_part = shifted(upward[:1], "lev", -1)
    return jnp.concatenate([upward[1:], level_part], axis=0)


def unroll_local(rolled, east_flag, north_flag, north_step):
    shift_cells = WIN // 2
    extent = rolled.shape[1]
    level_part = shifted(rolled[-1:], "lev", 1)
    upward = jnp.concatenate([level_part, rolled[:-1]], axis=0)
    north_part = upward[:, extent - shift_cells :]
    north_part = jnp.where(north_flag, north_part[:, :, ::-1], north_part)
    north_part = shifted(north_part, "tile", north_step)
    across = jnp.concatenate([north_part, upward[:, : extent - shift_cells]], axis=1)
    east_part = across[:, :, extent - shift_cells :]
    east_part = jnp.where(east_flag, east_part[:, ::-1], east_part)
    east_part = shifted(east_part, "tile", 1)
    return jnp.concatenate([east_part, across[:, :, : extent - shift_cells]], axis=2)


def to_windows(grid_field):
    levels = grid_field.shape[0]
    extent = grid_field.shape[1]
    channels = grid_field.shape[3]
    blocks = grid_field.reshape(
        levels // WIN_LEV, WIN_LEV, extent // WIN, WIN, extent // WIN, WIN, channels
    )
    blocks = blocks.transpose(0, 2, 4, 1, 3, 5, 6)
    return blocks.reshape(-1, WIN_LEV * WIN * WIN, channels)


def from_windows(windows, levels, extent):
    channels = windows.shape[-1]
    blocks = windows.reshape(
        levels // WIN_LEV, extent // WIN, extent // WIN, WIN_LEV, WIN, WIN, channels
    )
    blocks = blocks.transpose(0, 3, 1, 4, 2, 5, 6)
    return blocks.reshape(levels, extent, extent, channels)


def split_heads(packed):
    windows = packed.shape[0]
    tokens = packed.shape[1]
    model_width = packed.shape[2] // 3
    head_count = model_width // HEAD_DIM
    query_part = packed[:, :, :model_width].reshape(windows, tokens, head_count, HEAD_DIM)
    key_part = packed[:, :, model_width : 2 * model_width].reshape(
        windows, tokens, head_count, HEAD_DIM
    )
    value_part = packed[:, :, 2 * model_width :].reshape(windows, tokens, head_count, HEAD_DIM)
    return (query_part, key_part, value_part)


def window_mask(wrap_flags, tokens):
    level_of = jnp.arange(tokens, dtype=jnp.int32) // (WIN * WIN)
    same_level = level_of[:, None] == level_of[None, :]
    allowed = jnp.logical_or(
        same_level[None, None], jnp.logical_not(wrap_flags)[:, None, None, None]
    )
    return allowed.astype(jnp.float32)


def attend_forward(packed, wrap_flags):
    query_part, key_part, value_part = split_heads(packed)
    scores = jnp.einsum(
        "wqhd,wkhd->whqk", query_part, key_part, preferred_element_type=jnp.float32
    ) * HEAD_DIM ** (-0.5)
    raised = jnp.exp(scores) * window_mask(wrap_flags, packed.shape[1])
    prob = raised / jnp.sum(raised, axis=-1, keepdims=True)
    prob_low = prob.astype(jnp.bfloat16)
    attended = jnp.einsum(
        "whqk,wkhd->wqhd", prob_low, value_part, preferred_element_type=jnp.float32
    )
    attended = attended.astype(jnp.bfloat16).reshape(packed.shape[0], packed.shape[1], -1)
    return (attended, prob, prob_low)


def attend_backward(packed, back_windows, prob, prob_low):
    query_part, key_part, value_part = split_heads(packed)
    back_heads = back_windows.reshape(query_part.shape)
    grad_value = jnp.einsum(
        "whqk,wqhd->wkhd", prob_low, back_heads, preferred_element_type=jnp.float32
    )
    grad_prob = jnp.einsum(
        "wqhd,wkhd->whqk", back_heads, value_part, preferred_element_type=jnp.float32
    )
    centre = jnp.sum(prob * grad_prob, axis=-1, keepdims=True)
    grad_scores = (prob * (grad_prob - centre) * HEAD_DIM ** (-0.5)).astype(jnp.bfloat16)
    grad_query = jnp.einsum(
        "whqk,wkhd->wqhd", grad_scores, key_part, preferred_element_type=jnp.float32
    )
    grad_key = jnp.einsum(
        "whqk,wqhd->wkhd", grad_scores, query_part, preferred_element_type=jnp.float32
    )
    windows = packed.shape[0]
    tokens = packed.shape[1]
    joined = jnp.concatenate(
        [
            grad_query.reshape(windows, tokens, -1),
            grad_key.reshape(windows, tokens, -1),
            grad_value.reshape(windows, tokens, -1),
        ],
        axis=-1,
    )
    return joined.astype(jnp.bfloat16)


def shards_general(tokens, w_qkv, w_proj, seam_codes, upstream):
    levels = tokens.shape[1]
    extent = tokens.shape[3]
    model_width = tokens.shape[5]
    tiles_count = lax.axis_size("tile")
    north_step = tiles_count // 4
    tile_here = lax.axis_index("tile")
    east_flag = seam_codes[tile_here, 0] == 1
    north_flag = seam_codes[tile_here, 1] == 1
    top_level = lax.axis_index("lev") == lax.axis_size("lev") - 1
    per_level = extent // WIN * (extent // WIN)
    window_total = levels // WIN_LEV * per_level
    lev_window = jnp.arange(window_total, dtype=jnp.int32) // per_level
    wrap_flags = jnp.logical_and(top_level, lev_window == levels // WIN_LEV - 1)
    contract_last = (((1,), (1,)), ((), ()))
    contract_first = (((0,), (0,)), ((), ()))
    grid_in = tokens.reshape(levels, extent, extent, model_width)
    grid_up = upstream.reshape(levels, extent, extent, model_width)
    paired = roll_local(
        jnp.concatenate([grid_in, grid_up], axis=-1), east_flag, north_flag, north_step
    )
    grid_in = paired[..., :model_width]
    grid_up = paired[..., model_width:]
    token_rows = grid_in.reshape(-1, model_width)
    upstream_rows = grid_up.reshape(-1, model_width)
    normalized, inverse = layer_stats(token_rows)
    hidden = normalized.astype(jnp.bfloat16)
    full_qkv, full_proj = (
        lax.all_gather(w_qkv, "tile", axis=0, tiled=True),
        lax.all_gather(w_proj, "tile", axis=0, tiled=True),
    )
    projected = jnp.dot(hidden, full_qkv, preferred_element_type=jnp.float32).astype(jnp.bfloat16)
    grid_qkv = projected.reshape(levels, extent, extent, 3 * model_width)
    windows_qkv = to_windows(grid_qkv)
    attended, prob, prob_low = attend_forward(windows_qkv, wrap_flags)
    grid_mixed = from_windows(attended, levels, extent)
    mixed_in = grid_mixed.reshape(-1, model_width)
    mixed_out = lax.dot_general(
        mixed_in, full_proj, contract_last, preferred_element_type=jnp.float32
    )
    back_mix = jnp.dot(upstream_rows, full_proj, preferred_element_type=jnp.float32)
    output_low = (token_rows.astype(jnp.float32) + mixed_out).astype(jnp.bfloat16)
    back_low = back_mix.astype(jnp.bfloat16)
    grid_back = back_low.reshape(levels, extent, extent, model_width)
    grad_windows = attend_backward(windows_qkv, to_windows(grid_back), prob, prob_low)
    grid_grad = from_windows(grad_windows, levels, extent)
    grad_qkv_tok = grid_grad.reshape(-1, 3 * model_width)
    grad_hidden = lax.dot_general(
        grad_qkv_tok, full_qkv, contract_last, preferred_element_type=jnp.float32
    )
    grad_low = norm_backward(upstream_rows, grad_hidden, normalized, inverse)
    grid_output = output_low.reshape(levels, extent, extent, model_width)
    grid_dx = grad_low.reshape(levels, extent, extent, model_width)
    paired = unroll_local(
        jnp.concatenate([grid_output, grid_dx], axis=-1), east_flag, north_flag, north_step
    )
    grid_output = paired[..., :model_width]
    grid_dx = paired[..., model_width:]
    columns = hidden
    share_qkv = lax.psum_scatter(
        lax.dot_general(
            columns, grad_qkv_tok, contract_first, preferred_element_type=jnp.float32
        ).astype(jnp.bfloat16),
        "tile",
        scatter_dimension=0,
        tiled=True,
    )
    columns = upstream_rows
    share_proj = lax.psum_scatter(
        lax.dot_general(
            columns, mixed_in, contract_first, preferred_element_type=jnp.float32
        ).astype(jnp.bfloat16),
        "tile",
        scatter_dimension=0,
        tiled=True,
    )
    grad_qkv, grad_proj = (
        lax.psum(share_qkv, ("rep", "lev")).astype(jnp.float32),
        lax.psum(share_proj, ("rep", "lev")).astype(jnp.float32),
    )
    return (grid_output.reshape(tokens.shape), grid_dx.reshape(tokens.shape), grad_qkv, grad_proj)


LANES = 128
MAIN_MEBIBYTES = 56
NEAR = LANES // HEAD_DIM


def swapped(value, axis, mask):
    count = lax.axis_size(axis)
    return lax.ppermute(value, axis, [(source, source ^ mask) for source in range(count)])


def roll_source(codes_ref, cell, tile_here, tiles_count, extent):
    half = WIN // 2
    north_step = tiles_count // 4
    slot = cell // (extent * extent)
    row = (cell // extent) % extent
    col = cell % extent

    def code_of(tile, which):
        found = jnp.zeros_like(tile)
        for t in range(tiles_count):
            found = jnp.where(tile == t, codes_ref[t, which], found)
        return found == 1

    tile = jnp.bitwise_xor(slot, tile_here)
    crossed = row >= extent - half
    col1 = jnp.where(crossed & code_of(tile, 1), extent - 1 - col, col)
    row1 = jnp.where(crossed, row - (extent - half), row + half)
    tile1 = jnp.where(crossed, (tile + north_step) % tiles_count, tile)
    crossed = col1 >= extent - half
    row2 = jnp.where(crossed & code_of(tile1, 0), extent - 1 - row1, row1)
    col2 = jnp.where(crossed, col1 - (extent - half), col1 + half)
    tile2 = jnp.where(crossed, (tile1 + 1) % tiles_count, tile1)
    return (jnp.bitwise_xor(tile2, tile_here) * extent + row2) * extent + col2


def in_order(slots, here):
    bit = 1
    while bit < len(slots):
        odd = jnp.bitwise_and(here, bit) != 0
        slots = [jnp.where(odd, slots[k ^ bit], slots[k]) for k in range(len(slots))]
        bit *= 2
    return slots


def dot_nn(a, b):
    return lax.dot_general(a, b, (((1,), (0,)), ((), ())), preferred_element_type=jnp.float32)


def dot_nt(a, b):
    return lax.dot_general(a, b, (((1,), (1,)), ((), ())), preferred_element_type=jnp.float32)


def dot_tn(a, b):
    return lax.dot_general(a, b, (((0,), (0,)), ((), ())), preferred_element_type=jnp.float32)


def deal_kernel(qkv_any, out_any, in_any, up_any, high_ref, low_ref, *refs):
    *block_refs, qkv_ref, out_ref, sems = refs
    tiles_count = len(block_refs)
    channels = out_ref.shape[1]
    own = channels // tiles_count
    rep, here = lax.axis_index("rep"), lax.axis_index("tile")
    copies = [
        pltpu.make_async_copy(source.at[level], target.at[:, first : first + channels], sems.at[2 * level + which])
        for level, target in ((0, low_ref), (1, high_ref))
        for which, (source, first) in enumerate(((in_any, 0), (up_any, channels)))
    ]
    copies.append(pltpu.make_async_copy(qkv_any, qkv_ref, sems.at[4]))
    copies.append(pltpu.make_async_copy(out_any, out_ref, sems.at[5]))
    for copy in copies:
        copy.start()
    for copy in copies:
        copy.wait()

    def columns(which, tile):
        ref = out_ref if which == 3 else qkv_ref
        base = (0 if which == 3 else which * channels) + tile * own
        return ref[:, base : base + LANES], ref[:, base + LANES : base + own]

    blocks = []
    for tile in range(tiles_count):
        (q, q1), (k, k1), (v, v1), (p, p1) = [columns(which, tile) for which in range(4)]
        blocks.append(jnp.concatenate([q, k, q1, k1, v, p, v1, p1], axis=1))
    for slot, (ref, block) in enumerate(zip(block_refs, in_order(blocks, here))):
        if slot >= 2:
            half = block.shape[0] // 2
            block = jnp.where(rep == 0, block[:half], block[half:])
        ref[...] = block


def attend_window(block, allowed):
    tokens = block.shape[0]
    lane = lax.broadcasted_iota(jnp.int32, (1, LANES), 1)
    group = [block[:, g * LANES : (g + 1) * LANES] for g in range(6)]
    scale = HEAD_DIM ** (-0.5)

    def turned(x):
        return pltpu.roll(x.astype(jnp.float32), LANES // 2, 1)

    def attend(q, k, v, o, heads):
        masks = [lane // HEAD_DIM == h for h in range(heads)]

        def stacked(x):
            return jnp.concatenate([jnp.where(m, x, jnp.zeros_like(x)) for m in masks], axis=0)

        def folded(x):
            total = jnp.where(masks[0], x[:tokens], 0.0)
            for h in range(1, heads):
                total = jnp.where(masks[h], x[h * tokens : (h + 1) * tokens], total)
            return total

        k_all, v_all = stacked(k), stacked(v)
        scores = (dot_nt(k_all, q) * scale).reshape(heads, tokens, tokens)
        raised = jnp.exp(scores) * allowed[None]
        prob = raised / jnp.sum(raised, axis=1, keepdims=True)
        grad_prob = dot_nt(v_all, o).reshape(heads, tokens, tokens)
        centre = jnp.sum(prob * grad_prob, axis=1, keepdims=True)
        grad_scores = (prob * (grad_prob - centre) * scale).astype(jnp.bfloat16).reshape(-1, tokens)
        prob_low = prob.astype(jnp.bfloat16).reshape(-1, tokens)
        att = dot_tn(prob_low, v_all)
        grad_q = dot_tn(grad_scores, k_all)
        grad_k = folded(dot_nn(grad_scores, q))
        grad_v = folded(dot_nn(prob_low, o))
        return grad_q, grad_k, grad_v, att

    gq, gk, gv, att = attend(group[0], group[1], group[3], group[4], NEAR)
    qk_turned = turned(group[2]).astype(jnp.bfloat16)
    vo_turned = turned(group[5]).astype(jnp.bfloat16)
    gq1, gk1, gv1, att1 = attend(group[2], qk_turned, group[5], vo_turned, NEAR // 2)
    parts = [gq, gk, gq1 + turned(gk1), gv, att, gv1 + turned(att1)]
    return jnp.concatenate(parts, axis=1).astype(jnp.bfloat16)


def main_kernel(codes_ref, *refs):
    *refs, inner_ref, outer_ref, wts, keep_a, send_a, keep_b, send_b, hid, up, rolled, result, fields, sems = refs
    tiles_count = (len(refs) + 2) // 4
    cells_refs = refs[: 2 * tiles_count]
    near_refs = refs[2 * tiles_count : 2 * tiles_count + 2]
    far_refs = refs[2 * tiles_count + 2 :]
    cells = cells_refs[0].shape[0]
    channels = wts.shape[0]
    rows = channels // tiles_count
    half = rows // 2
    plane = tiles_count * cells
    rep, here = lax.axis_index("rep"), lax.axis_index("tile")
    unwrapped = lax.axis_index("lev") != lax.axis_size("lev") - 1
    copies = []

    def fetch(source, target):
        copy = pltpu.make_async_copy(source, target, sems.at[len(copies)])
        copy.start()
        copies.append(copy)

    for k in range(tiles_count):
        for l in range(2):
            fetch(cells_refs[2 * k + l], fields.at[pl.ds(l * plane + k * cells, cells)])
    for k in range(tiles_count):
        base = (here ^ k) * rows
        if k < 2:
            fetch(near_refs[k], wts.at[pl.ds(pl.multiple_of(base, 32), rows)])
        else:
            fetch(far_refs[2 * k - 4], wts.at[pl.ds(pl.multiple_of(base + rep * half, 32), half)])
            fetch(far_refs[2 * k - 3], wts.at[pl.ds(pl.multiple_of(base + (1 - rep) * half, 32), half)])
    for copy in copies[: 2 * tiles_count]:
        copy.wait()
    for at in range(0, 2 * plane, cells):
        x = fields[at : at + cells, :channels].astype(jnp.float32)
        center = jnp.mean(x, axis=1, keepdims=True)
        x = x - center
        spread = jnp.mean(jnp.square(x), axis=1, keepdims=True)
        hid[at : at + cells, :] = (x * lax.rsqrt(spread + EPSILON)).astype(jnp.bfloat16)
        up[at : at + cells, :] = fields[at : at + cells, channels:]
    for copy in copies[2 * tiles_count :]:
        copy.wait()

    lane = lax.broadcasted_iota(jnp.int32, (1, LANES), 1)
    low = lane < LANES // 2
    split = 4 * LANES
    extent = WIN
    source = roll_source(codes_ref, lax.broadcasted_iota(jnp.int32, (plane, 1), 0), here, tiles_count, extent)
    from_col = lax.broadcasted_iota(jnp.int32, (plane, plane), 1) == source
    selector = jnp.where(from_col, 1.0, 0.0).astype(jnp.bfloat16)
    source = roll_source(codes_ref, lax.broadcasted_iota(jnp.int32, (1, plane), 1), here, tiles_count, extent)
    from_row = lax.broadcasted_iota(jnp.int32, (plane, plane), 0) == source
    back_selector = jnp.where(from_row, 1.0, 0.0).astype(jnp.bfloat16)
    for l in range(2):
        at = slice(l * plane, (l + 1) * plane)
        front = dot_nn(hid[at, :], wts[:, :split])
        last = dot_nn(hid[at, :], wts[:, split + LANES :])
        back = dot_nn(up[at, :], wts[:, split:])
        mixed = jnp.where(low, last, back[:, LANES:])
        whole = jnp.concatenate([front, back[:, :LANES], mixed], axis=1).astype(jnp.bfloat16)
        rolled[l] = dot_nn(selector, whole).astype(jnp.bfloat16)

    tokens = 2 * cells
    level_k = lax.broadcasted_iota(jnp.int32, (tokens, tokens), 0) // cells
    level_q = lax.broadcasted_iota(jnp.int32, (tokens, tokens), 1) // cells
    allowed = jnp.where((level_k == level_q) | unwrapped, 1.0, 0.0)

    def window(w, carry):
        at = pl.ds(pl.multiple_of(w * cells, cells), cells)
        block = jnp.concatenate([rolled[0, at, :], rolled[1, at, :]], axis=0)
        out = attend_window(block, allowed)
        result[0, at, :] = out[:cells]
        result[1, at, :] = out[cells:]
        return carry

    lax.fori_loop(0, tiles_count, window, 0)

    zero = jnp.zeros((plane, LANES), jnp.bfloat16)
    for l in range(2):
        at = slice(l * plane, (l + 1) * plane)
        tok = dot_nn(back_selector, result[l]).astype(jnp.bfloat16)
        tail = tok[:, split + LANES :]
        inner_ref[at, :] = jnp.concatenate([tok[:, :split], zero, jnp.where(low, tail, zero)], axis=1)
        outer_ref[at, :] = jnp.concatenate([tok[:, split : split + LANES], jnp.where(low, zero, tail)], axis=1)
    inner, outer = inner_ref[...], outer_ref[...]
    hid_t = hid[...].T
    up_t = up[...].T
    width = 3 * LANES
    share_b = dot_nn(hid_t, inner[:, width:])
    share_b = jnp.concatenate(
        [share_b[:, :LANES], share_b[:, LANES:] + dot_nn(up_t, outer)], axis=1
    ).astype(jnp.bfloat16)
    share_a = dot_nn(hid_t, inner[:, :width]).astype(jnp.bfloat16)
    for share, keep, send in ((share_b, keep_b, send_b), (share_a, keep_a, send_a)):
        for j in range(tiles_count):
            first = share[j * rows : j * rows + half]
            second = share[j * rows + half : (j + 1) * rows]
            keep[j] = jnp.where(rep == 0, first, second)
            send[j] = jnp.where(rep == 0, second, first)


def rows_kernel(inner_ref, outer_ref, wts, keep_ref, send_ref):
    slots, levels, cells, width = keep_ref.shape
    channels = width // 2
    plane = 2 * slots * cells
    split = 4 * LANES
    for l in range(levels):
        at = slice(l * plane, (l + 1) * plane)
        grad_hidden = dot_nt(inner_ref[at, :], wts[...]).astype(jnp.bfloat16)
        mixed_out = dot_nt(outer_ref[at, :], wts[:, split:]).astype(jnp.bfloat16)
        for k in range(2 * slots):
            ref = send_ref if k % 2 else keep_ref
            at = slice(k * cells, (k + 1) * cells)
            ref[k // 2, l, :, :channels] = mixed_out[at]
            ref[k // 2, l, :, channels:] = grad_hidden[at]


def column_kernel(*refs):
    *slot_refs, out_ref = refs
    here = lax.axis_index("tile")
    blocks = in_order([ref[...] for ref in slot_refs], here)
    pieces = []
    for which in range(2):
        for block in blocks:
            pieces.append(block[:, which * LANES : (which + 1) * LANES])
            rest = 2 * LANES + which * (LANES // 2)
            pieces.append(block[:, rest : rest + LANES // 2])
    out_ref[...] = jnp.concatenate(pieces, axis=1)


SMEM_SPEC = pl.BlockSpec(memory_space=pltpu.SMEM)
VMEM_SPEC = pl.BlockSpec(memory_space=pltpu.VMEM)
ANY_SPEC = pl.BlockSpec(memory_space=pl.ANY)


def call(body, outs, scalars, arrays, flops, mebibytes, scratch=(), spec=VMEM_SPEC):
    moved = sum(a.size * a.dtype.itemsize for a in arrays) + sum(o.size * o.dtype.itemsize for o in outs)
    return pl.pallas_call(
        body,
        out_shape=outs,
        in_specs=[SMEM_SPEC] * len(scalars) + [spec] * len(arrays),
        out_specs=[VMEM_SPEC] * len(outs),
        scratch_shapes=list(scratch),
        compiler_params=pltpu.CompilerParams(vmem_limit_bytes=mebibytes * 1024 * 1024),
        cost_estimate=pl.CostEstimate(flops=flops, bytes_accessed=moved, transcendentals=0),
    )(*scalars, *arrays)


def low_shape(*shape):
    return jax.ShapeDtypeStruct(shape, jnp.bfloat16)


def added(a, b):
    return (a.astype(jnp.float32) + b.astype(jnp.float32)).astype(jnp.bfloat16)


def parted(value, dim, bit):
    size = value.shape[dim] // 2
    keep = lax.dynamic_slice_in_dim(value, bit * size, size, dim)
    send = lax.dynamic_slice_in_dim(value, (1 - bit) * size, size, dim)
    return keep, send


def joined(mine, other, bit, dim=0):
    odd = bit == 1
    return jnp.concatenate([jnp.where(odd, other, mine), jnp.where(odd, mine, other)], axis=dim)


def bits_of(count):
    bits, bit = [], 1
    while bit < count:
        bits.append(bit)
        bit *= 2
    return bits


def reduce_share(keep, send, lev_here, tile_here):
    came = swapped(send, "rep", 1)
    part = added(keep, came)
    for bit in bits_of(lax.axis_size("lev")):
        keep, send = parted(part, 1, (lev_here // bit) % 2)
        came = swapped(send, "lev", bit)
        part = added(keep, came)
    tiles_count = lax.axis_size("tile")
    near = tile_here % 2
    pairs = part.reshape(tiles_count // 2, 2, *part.shape[1:])
    mine = lax.dynamic_index_in_dim(pairs, near, 1, keepdims=False)
    away = lax.dynamic_index_in_dim(pairs, 1 - near, 1, keepdims=False)
    came = swapped(away, "tile", 1)
    both = jnp.stack([mine, came], axis=1)
    far = tile_here // 2
    slots = lax.dynamic_index_in_dim(both, far, 0, keepdims=False)
    found = [slots[0], slots[1]]
    for mask in range(1, tiles_count // 2):
        got = swapped(lax.dynamic_index_in_dim(both, far ^ mask, 0, keepdims=False), "tile", 2 * mask)
        found += [got[0], got[1]]
    rows, cols = part.shape[1:]
    channels = tiles_count * cols // 2
    return call(column_kernel, [low_shape(rows, 2 * channels)], [], found, 1000, 4)[0]


def spread(piece, lev_here):
    for bit in reversed(bits_of(lax.axis_size("lev"))):
        came = swapped(piece, "lev", bit)
        piece = joined(piece, came, (lev_here // bit) % 2)
    came = swapped(piece, "rep", 1)
    return piece, came


def shards_by_heads(tokens, w_qkv, w_proj, seam_codes, upstream):
    levels, extent, channels = tokens.shape[1], tokens.shape[3], tokens.shape[5]
    cells = extent * extent
    tiles_count = lax.axis_size("tile")
    rep_here, lev_here, tile_here = lax.axis_index("rep"), lax.axis_index("lev"), lax.axis_index("tile")
    shard_rows = w_qkv.shape[0]
    field_in = tokens.reshape(levels, cells, channels)
    field_up = upstream.reshape(levels, cells, channels)
    half = shard_rows // 2

    shape = low_shape(cells, 2 * channels)
    high, low, *blocks = call(
        deal_kernel,
        [shape, shape]
        + [low_shape(shard_rows, channels)] * 2
        + [low_shape(half, channels)] * (tiles_count - 2),
        [],
        [w_qkv, w_proj, field_in, field_up],
        1000,
        MAIN_MEBIBYTES,
        scratch=[
            pltpu.VMEM(w_qkv.shape, jnp.bfloat16),
            pltpu.VMEM(w_proj.shape, jnp.bfloat16),
            pltpu.SemaphoreType.DMA((6,)),
        ],
        spec=ANY_SPEC,
    )
    low = shifted(low, "lev", -1)
    weights = [blocks[0]]
    for k in range(1, tiles_count):
        weights.append(swapped(blocks[k], "tile", k))
        if k >= 2:
            weights.append(swapped(weights[-1], "rep", 1))

    def gathered(piece):
        have = {0: piece}
        for bit in reversed(bits_of(tiles_count)):
            for k in list(have):
                have[k ^ bit] = swapped(have[k], "tile", bit)
        return [have[k] for k in range(tiles_count)]

    pieces = [p for pair in zip(gathered(high), gathered(low)) for p in pair]
    plane = tiles_count * cells
    width = 3 * LANES
    part_shape = low_shape(tiles_count, half, width)
    inner_shape = low_shape(levels * plane, 2 * width)
    outer_shape = low_shape(levels * plane, 2 * LANES)
    weight_shape = low_shape(channels, 2 * width)
    inner, outer, weight, keep_a, send_a, keep_b, send_b = call(
        main_kernel,
        [inner_shape, outer_shape, weight_shape, part_shape, part_shape, part_shape, part_shape],
        [seam_codes],
        [*pieces, *weights],
        8 * levels * plane * channels * channels,
        MAIN_MEBIBYTES,
        scratch=[
            pltpu.VMEM((levels * plane, channels), jnp.bfloat16),
            pltpu.VMEM((levels * plane, channels), jnp.bfloat16),
            pltpu.VMEM((levels, plane, 2 * width), jnp.bfloat16),
            pltpu.VMEM((levels, plane, 2 * width), jnp.bfloat16),
            pltpu.VMEM((levels * plane, 2 * channels), jnp.bfloat16),
            pltpu.SemaphoreType.DMA((len(pieces) + len(weights),)),
        ],
        spec=ANY_SPEC,
    )
    sums_shape = low_shape(tiles_count // 2, levels, cells, 2 * channels)
    keep, send = call(rows_kernel, [sums_shape, sums_shape], [], [inner, outer, weight], 10**9, 16)

    came = swapped(send, "tile", 1)
    sums = added(keep, came)
    slots = [sums[k] for k in range(tiles_count // 2)]
    for bit in bits_of(tiles_count // 2):
        came = swapped(jnp.stack(slots[1::2]), "tile", 2 * bit)
        slots = [added(slots[2 * k], came[k]) for k in range(len(slots) // 2)]
    final = slots[0]
    low_back = shifted(final[1], "lev", 1)
    final = jnp.stack([low_back, final[0]]).reshape(levels * cells, 2 * channels)
    token_rows = field_in.reshape(-1, channels)
    upstream_rows = field_up.reshape(-1, channels)
    normalized, inverse = layer_stats(token_rows)
    output = (token_rows.astype(jnp.float32) + final[:, :channels].astype(jnp.float32)).astype(jnp.bfloat16)
    grad_tokens = norm_backward(upstream_rows, final[:, channels:].astype(jnp.float32), normalized, inverse)

    (own_b, other_b), (own_a, other_a) = [
        spread(reduce_share(*pair, level, tile), level)
        for pair, (level, tile) in (
            ((keep_b, send_b), (lev_here, tile_here)),
            ((keep_a, send_a), lax.optimization_barrier((lev_here, tile_here))),
        )
    ]
    rows = own_a.shape[0]
    grad_qkv = jnp.zeros((shard_rows, 3 * channels), jnp.float32)
    grad_proj = jnp.zeros((shard_rows, channels), jnp.float32)
    for piece_a, piece_b, at in ((own_a, own_b, rep_here * rows), (other_a, other_b, (1 - rep_here) * rows)):
        value, out = piece_b[:, :channels].astype(jnp.float32), piece_b[:, channels:].astype(jnp.float32)
        grad_proj = lax.dynamic_update_slice(grad_proj, out, (at, 0))
        grad_qkv = lax.dynamic_update_slice(grad_qkv, value, (at, 2 * channels))
        grad_qkv = lax.dynamic_update_slice(grad_qkv, piece_a.astype(jnp.float32), (at, 0))
    return (output.reshape(tokens.shape), grad_tokens.reshape(tokens.shape), grad_qkv, grad_proj)


def power_of_two(count):
    return count & (count - 1) == 0


def shards(tokens, w_qkv, w_proj, seam_codes, upstream):
    counts = [lax.axis_size(axis) for axis in ("rep", "lev", "tile")]
    tiles_count = counts[2]
    channels = tokens.shape[5]
    one_window = tokens.shape[0] == 1 and tokens.shape[1] == WIN_LEV and tokens.shape[3] == WIN and tokens.shape[2] == 1
    by_heads = (
        one_window
        and all(power_of_two(count) for count in counts)
        and tiles_count % 4 == 0
        and (channels // HEAD_DIM) % tiles_count == 0
        and channels // tiles_count == LANES + LANES // 2
        and counts[0] == 2
        and (channels // tiles_count) % (8 * counts[0] * counts[1]) == 0
    )
    if not by_heads:
        return shards_general(tokens, w_qkv, w_proj, seam_codes, upstream)
    return shards_by_heads(tokens, w_qkv, w_proj, seam_codes, upstream)


def solution(mesh):
    in_specs = (
        P("rep", "lev", "tile", None, None, None),
        P("tile", None),
        P("tile", None),
        P(),
        P("rep", "lev", "tile", None, None, None),
    )
    out_specs = (
        P("rep", "lev", "tile", None, None, None),
        P("rep", "lev", "tile", None, None, None),
        P("tile", None),
        P("tile", None),
    )
    return jax.shard_map(shards, mesh=mesh, in_specs=in_specs, out_specs=out_specs, check_vma=False)
```

```python
import jax
import jax.numpy as jnp
from jax import lax
from jax.experimental import pallas as pl
from jax.experimental.pallas import tpu as pltpu
from jax.sharding import PartitionSpec as P

HEAD_DIM = 32
WIN = 8
WIN_LEV = 2


EPSILON = 1e-05


def shifted(value, axis, steps):
    count = lax.axis_size(axis)
    pairs = [(source, (source + steps) % count) for source in range(count)]
    return lax.ppermute(value, axis, pairs)


def layer_stats(token_rows):
    values = token_rows.astype(jnp.float32)
    center = jnp.mean(values, axis=1, keepdims=True)
    spread = jnp.mean(jnp.square(values - center), axis=1, keepdims=True)
    inverse = lax.rsqrt(spread + EPSILON)
    return ((values - center) * inverse, inverse)


def norm_backward(upstream_rows, grad_hidden, normalized, inverse):
    centre = jnp.mean(grad_hidden, axis=1, keepdims=True)
    projected = jnp.mean(grad_hidden * normalized, axis=1, keepdims=True)
    total_grad = (
        upstream_rows.astype(jnp.float32)
        + (grad_hidden - centre - normalized * projected) * inverse
    )
    return total_grad.astype(jnp.bfloat16)


def roll_local(grid_field, east_flag, north_flag, north_step):
    shift_cells = WIN // 2
    east_part = shifted(grid_field[:, :, :shift_cells], "tile", -1)
    east_part = jnp.where(east_flag, east_part[:, ::-1], east_part)
    across = jnp.concatenate([grid_field[:, :, shift_cells:], east_part], axis=2)
    north_part = shifted(across[:, :shift_cells], "tile", -north_step)
    north_part = jnp.where(north_flag, north_part[:, :, ::-1], north_part)
    upward = jnp.concatenate([across[:, shift_cells:], north_part], axis=1)
    level_part = shifted(upward[:1], "lev", -1)
    return jnp.concatenate([upward[1:], level_part], axis=0)


def unroll_local(rolled, east_flag, north_flag, north_step):
    shift_cells = WIN // 2
    extent = rolled.shape[1]
    level_part = shifted(rolled[-1:], "lev", 1)
    upward = jnp.concatenate([level_part, rolled[:-1]], axis=0)
    north_part = upward[:, extent - shift_cells :]
    north_part = jnp.where(north_flag, north_part[:, :, ::-1], north_part)
    north_part = shifted(north_part, "tile", north_step)
    across = jnp.concatenate([north_part, upward[:, : extent - shift_cells]], axis=1)
    east_part = across[:, :, extent - shift_cells :]
    east_part = jnp.where(east_flag, east_part[:, ::-1], east_part)
    east_part = shifted(east_part, "tile", 1)
    return jnp.concatenate([east_part, across[:, :, : extent - shift_cells]], axis=2)


def to_windows(grid_field):
    levels = grid_field.shape[0]
    extent = grid_field.shape[1]
    channels = grid_field.shape[3]
    blocks = grid_field.reshape(
        levels // WIN_LEV, WIN_LEV, extent // WIN, WIN, extent // WIN, WIN, channels
    )
    blocks = blocks.transpose(0, 2, 4, 1, 3, 5, 6)
    return blocks.reshape(-1, WIN_LEV * WIN * WIN, channels)


def from_windows(windows, levels, extent):
    channels = windows.shape[-1]
    blocks = windows.reshape(
        levels // WIN_LEV, extent // WIN, extent // WIN, WIN_LEV, WIN, WIN, channels
    )
    blocks = blocks.transpose(0, 3, 1, 4, 2, 5, 6)
    return blocks.reshape(levels, extent, extent, channels)


def split_heads(packed):
    windows = packed.shape[0]
    tokens = packed.shape[1]
    model_width = packed.shape[2] // 3
    head_count = model_width // HEAD_DIM
    query_part = packed[:, :, :model_width].reshape(windows, tokens, head_count, HEAD_DIM)
    key_part = packed[:, :, model_width : 2 * model_width].reshape(
        windows, tokens, head_count, HEAD_DIM
    )
    value_part = packed[:, :, 2 * model_width :].reshape(windows, tokens, head_count, HEAD_DIM)
    return (query_part, key_part, value_part)


def window_mask(wrap_flags, tokens):
    level_of = jnp.arange(tokens, dtype=jnp.int32) // (WIN * WIN)
    same_level = level_of[:, None] == level_of[None, :]
    allowed = jnp.logical_or(
        same_level[None, None], jnp.logical_not(wrap_flags)[:, None, None, None]
    )
    return allowed.astype(jnp.float32)


def attend_forward(packed, wrap_flags):
    query_part, key_part, value_part = split_heads(packed)
    scores = jnp.einsum(
        "wqhd,wkhd->whqk", query_part, key_part, preferred_element_type=jnp.float32
    ) * HEAD_DIM ** (-0.5)
    raised = jnp.exp(scores) * window_mask(wrap_flags, packed.shape[1])
    prob = raised / jnp.sum(raised, axis=-1, keepdims=True)
    prob_low = prob.astype(jnp.bfloat16)
    attended = jnp.einsum(
        "whqk,wkhd->wqhd", prob_low, value_part, preferred_element_type=jnp.float32
    )
    attended = attended.astype(jnp.bfloat16).reshape(packed.shape[0], packed.shape[1], -1)
    return (attended, prob, prob_low)


def attend_backward(packed, back_windows, prob, prob_low):
    query_part, key_part, value_part = split_heads(packed)
    back_heads = back_windows.reshape(query_part.shape)
    grad_value = jnp.einsum(
        "whqk,wqhd->wkhd", prob_low, back_heads, preferred_element_type=jnp.float32
    )
    grad_prob = jnp.einsum(
        "wqhd,wkhd->whqk", back_heads, value_part, preferred_element_type=jnp.float32
    )
    centre = jnp.sum(prob * grad_prob, axis=-1, keepdims=True)
    grad_scores = (prob * (grad_prob - centre) * HEAD_DIM ** (-0.5)).astype(jnp.bfloat16)
    grad_query = jnp.einsum(
        "whqk,wkhd->wqhd", grad_scores, key_part, preferred_element_type=jnp.float32
    )
    grad_key = jnp.einsum(
        "whqk,wqhd->wkhd", grad_scores, query_part, preferred_element_type=jnp.float32
    )
    windows = packed.shape[0]
    tokens = packed.shape[1]
    joined = jnp.concatenate(
        [
            grad_query.reshape(windows, tokens, -1),
            grad_key.reshape(windows, tokens, -1),
            grad_value.reshape(windows, tokens, -1),
        ],
        axis=-1,
    )
    return joined.astype(jnp.bfloat16)


def shards_general(tokens, w_qkv, w_proj, seam_codes, upstream):
    levels = tokens.shape[1]
    extent = tokens.shape[3]
    model_width = tokens.shape[5]
    tiles_count = lax.axis_size("tile")
    north_step = tiles_count // 4
    tile_here = lax.axis_index("tile")
    east_flag = seam_codes[tile_here, 0] == 1
    north_flag = seam_codes[tile_here, 1] == 1
    top_level = lax.axis_index("lev") == lax.axis_size("lev") - 1
    per_level = extent // WIN * (extent // WIN)
    window_total = levels // WIN_LEV * per_level
    lev_window = jnp.arange(window_total, dtype=jnp.int32) // per_level
    wrap_flags = jnp.logical_and(top_level, lev_window == levels // WIN_LEV - 1)
    contract_last = (((1,), (1,)), ((), ()))
    contract_first = (((0,), (0,)), ((), ()))
    grid_in = tokens.reshape(levels, extent, extent, model_width)
    grid_up = upstream.reshape(levels, extent, extent, model_width)
    paired = roll_local(
        jnp.concatenate([grid_in, grid_up], axis=-1), east_flag, north_flag, north_step
    )
    grid_in = paired[..., :model_width]
    grid_up = paired[..., model_width:]
    token_rows = grid_in.reshape(-1, model_width)
    upstream_rows = grid_up.reshape(-1, model_width)
    normalized, inverse = layer_stats(token_rows)
    hidden = normalized.astype(jnp.bfloat16)
    full_qkv, full_proj = (
        lax.all_gather(w_qkv, "tile", axis=0, tiled=True),
        lax.all_gather(w_proj, "tile", axis=0, tiled=True),
    )
    projected = jnp.dot(hidden, full_qkv, preferred_element_type=jnp.float32).astype(jnp.bfloat16)
    grid_qkv = projected.reshape(levels, extent, extent, 3 * model_width)
    windows_qkv = to_windows(grid_qkv)
    attended, prob, prob_low = attend_forward(windows_qkv, wrap_flags)
    grid_mixed = from_windows(attended, levels, extent)
    mixed_in = grid_mixed.reshape(-1, model_width)
    mixed_out = lax.dot_general(
        mixed_in, full_proj, contract_last, preferred_element_type=jnp.float32
    )
    back_mix = jnp.dot(upstream_rows, full_proj, preferred_element_type=jnp.float32)
    output_low = (token_rows.astype(jnp.float32) + mixed_out).astype(jnp.bfloat16)
    back_low = back_mix.astype(jnp.bfloat16)
    grid_back = back_low.reshape(levels, extent, extent, model_width)
    grad_windows = attend_backward(windows_qkv, to_windows(grid_back), prob, prob_low)
    grid_grad = from_windows(grad_windows, levels, extent)
    grad_qkv_tok = grid_grad.reshape(-1, 3 * model_width)
    grad_hidden = lax.dot_general(
        grad_qkv_tok, full_qkv, contract_last, preferred_element_type=jnp.float32
    )
    grad_low = norm_backward(upstream_rows, grad_hidden, normalized, inverse)
    grid_output = output_low.reshape(levels, extent, extent, model_width)
    grid_dx = grad_low.reshape(levels, extent, extent, model_width)
    paired = unroll_local(
        jnp.concatenate([grid_output, grid_dx], axis=-1), east_flag, north_flag, north_step
    )
    grid_output = paired[..., :model_width]
    grid_dx = paired[..., model_width:]
    columns = hidden
    share_qkv = lax.psum_scatter(
        lax.dot_general(
            columns, grad_qkv_tok, contract_first, preferred_element_type=jnp.float32
        ).astype(jnp.bfloat16),
        "tile",
        scatter_dimension=0,
        tiled=True,
    )
    columns = upstream_rows
    share_proj = lax.psum_scatter(
        lax.dot_general(
            columns, mixed_in, contract_first, preferred_element_type=jnp.float32
        ).astype(jnp.bfloat16),
        "tile",
        scatter_dimension=0,
        tiled=True,
    )
    grad_qkv, grad_proj = (
        lax.psum(share_qkv, ("rep", "lev")).astype(jnp.float32),
        lax.psum(share_proj, ("rep", "lev")).astype(jnp.float32),
    )
    return (grid_output.reshape(tokens.shape), grid_dx.reshape(tokens.shape), grad_qkv, grad_proj)


LANES = 128
MAIN_MEBIBYTES = 56
UNROLL = 4
NEAR = LANES // HEAD_DIM


def swapped(value, axis, mask):
    count = lax.axis_size(axis)
    return lax.ppermute(value, axis, [(source, source ^ mask) for source in range(count)])


def roll_source(codes_ref, cell, tile_here, tiles_count, extent):
    half = WIN // 2
    north_step = tiles_count // 4
    slot = cell // (extent * extent)
    row = (cell // extent) % extent
    col = cell % extent

    def code_of(tile, which):
        found = jnp.zeros_like(tile)
        for t in range(tiles_count):
            found = jnp.where(tile == t, codes_ref[2 * t + which], found)
        return found == 1

    tile = jnp.bitwise_xor(slot, tile_here)
    crossed = row >= extent - half
    col1 = jnp.where(crossed & code_of(tile, 1), extent - 1 - col, col)
    row1 = jnp.where(crossed, row - (extent - half), row + half)
    tile1 = jnp.where(crossed, (tile + north_step) % tiles_count, tile)
    crossed = col1 >= extent - half
    row2 = jnp.where(crossed & code_of(tile1, 0), extent - 1 - row1, row1)
    col2 = jnp.where(crossed, col1 - (extent - half), col1 + half)
    tile2 = jnp.where(crossed, (tile1 + 1) % tiles_count, tile1)
    return (jnp.bitwise_xor(tile2, tile_here) * extent + row2) * extent + col2


def in_order(slots, here):
    bit = 1
    while bit < len(slots):
        odd = jnp.bitwise_and(here, bit) != 0
        slots = [jnp.where(odd, slots[k ^ bit], slots[k]) for k in range(len(slots))]
        bit *= 2
    return slots


def dot_nn(a, b):
    return lax.dot_general(a, b, (((1,), (0,)), ((), ())), preferred_element_type=jnp.float32)


def dot_nt(a, b):
    return lax.dot_general(a, b, (((1,), (1,)), ((), ())), preferred_element_type=jnp.float32)


def dot_tn(a, b):
    return lax.dot_general(a, b, (((0,), (0,)), ((), ())), preferred_element_type=jnp.float32)


def deal_kernel(qkv_any, out_any, in_any, up_any, high_ref, low_ref, *refs):
    *block_refs, qkv_ref, out_ref, sems = refs
    tiles_count = len(block_refs)
    channels = out_ref.shape[1]
    own = channels // tiles_count
    rep, here = lax.axis_index("rep"), lax.axis_index("tile")
    copies = [
        pltpu.make_async_copy(source.at[level], target.at[:, first : first + channels], sems.at[2 * level + which])
        for level, target in ((0, low_ref), (1, high_ref))
        for which, (source, first) in enumerate(((in_any, 0), (up_any, channels)))
    ]
    copies.append(pltpu.make_async_copy(qkv_any, qkv_ref, sems.at[4]))
    copies.append(pltpu.make_async_copy(out_any, out_ref, sems.at[5]))
    for copy in copies:
        copy.start()
    for copy in copies:
        copy.wait()

    def columns(which, tile):
        ref = out_ref if which == 3 else qkv_ref
        base = (0 if which == 3 else which * channels) + tile * own
        return ref[:, base : base + LANES], ref[:, base + LANES : base + own]

    blocks = []
    for tile in range(tiles_count):
        (q, q1), (k, k1), (v, v1), (p, p1) = [columns(which, tile) for which in range(4)]
        blocks.append(jnp.concatenate([q, k, q1, k1, v, p, v1, p1], axis=1))
    for slot, (ref, block) in enumerate(zip(block_refs, in_order(blocks, here))):
        if slot >= 2:
            half = block.shape[0] // 2
            block = jnp.where(rep == 0, block[:half], block[half:])
        ref[...] = block


def attend_window(block, allowed):
    tokens = block.shape[0]
    lane = lax.broadcasted_iota(jnp.int32, (1, LANES), 1)
    group = [block[:, g * LANES : (g + 1) * LANES] for g in range(6)]
    scale = HEAD_DIM ** (-0.5)

    def turned(x):
        return pltpu.roll(x.astype(jnp.float32), LANES // 2, 1)

    def attend(q, k, v, o, heads):
        masks = [lane // HEAD_DIM == h for h in range(heads)]

        def stacked(x):
            return jnp.concatenate([jnp.where(m, x, jnp.zeros_like(x)) for m in masks], axis=0)

        def folded(x):
            total = jnp.where(masks[0], x[:tokens], 0.0)
            for h in range(1, heads):
                total = jnp.where(masks[h], x[h * tokens : (h + 1) * tokens], total)
            return total

        k_all, v_all = stacked(k), stacked(v)
        scores = (dot_nt(k_all, q) * scale).reshape(heads, tokens, tokens)
        raised = jnp.exp(scores) * allowed[None]
        prob = raised * (1.0 / jnp.sum(raised, axis=1, keepdims=True))
        grad_prob = dot_nt(v_all, o).reshape(heads, tokens, tokens)
        centre = jnp.sum(prob * grad_prob, axis=1, keepdims=True)
        grad_scores = (prob * (grad_prob - centre) * scale).astype(jnp.bfloat16).reshape(-1, tokens)
        prob_low = prob.astype(jnp.bfloat16).reshape(-1, tokens)
        att = dot_tn(prob_low, v_all)
        grad_q = dot_tn(grad_scores, k_all)
        grad_k = folded(dot_nn(grad_scores, q))
        grad_v = folded(dot_nn(prob_low, o))
        return grad_q, grad_k, grad_v, att

    gq, gk, gv, att = attend(group[0], group[1], group[3], group[4], NEAR)
    qk_turned = turned(group[2]).astype(jnp.bfloat16)
    vo_turned = turned(group[5]).astype(jnp.bfloat16)
    gq1, gk1, gv1, att1 = attend(group[2], qk_turned, group[5], vo_turned, NEAR // 2)
    parts = [gq, gk, gq1 + turned(gk1), gv, att, gv1 + turned(att1)]
    return jnp.concatenate(parts, axis=1).astype(jnp.bfloat16)


def main_kernel(codes_ref, *refs):
    *refs, inner_ref, outer_ref, wts, keep_a, send_a, keep_b, send_b, hid, up, rolled, result, fields, sems = refs
    tiles_count = (len(refs) + 2) // 4
    cells_refs = refs[: 2 * tiles_count]
    near_refs = refs[2 * tiles_count : 2 * tiles_count + 2]
    far_refs = refs[2 * tiles_count + 2 :]
    cells = cells_refs[0].shape[0]
    channels = wts.shape[0]
    rows = channels // tiles_count
    half = rows // 2
    plane = tiles_count * cells
    rep, here = lax.axis_index("rep"), lax.axis_index("tile")
    unwrapped = lax.axis_index("lev") != lax.axis_size("lev") - 1
    copies = []

    def fetch(source, target):
        copy = pltpu.make_async_copy(source, target, sems.at[len(copies)])
        copy.start()
        copies.append(copy)

    for k in range(tiles_count):
        for l in range(2):
            fetch(cells_refs[2 * k + l], fields.at[pl.ds(l * plane + k * cells, cells)])
    for k in range(tiles_count):
        base = (here ^ k) * rows
        if k < 2:
            fetch(near_refs[k], wts.at[pl.ds(pl.multiple_of(base, 32), rows)])
        else:
            fetch(far_refs[2 * k - 4], wts.at[pl.ds(pl.multiple_of(base + rep * half, 32), half)])
            fetch(far_refs[2 * k - 3], wts.at[pl.ds(pl.multiple_of(base + (1 - rep) * half, 32), half)])
    for copy in copies[: 2 * tiles_count]:
        copy.wait()
    for at in range(0, 2 * plane, cells):
        x = fields[at : at + cells, :channels].astype(jnp.float32)
        center = jnp.mean(x, axis=1, keepdims=True)
        x = x - center
        spread = jnp.mean(jnp.square(x), axis=1, keepdims=True)
        hid[at : at + cells, :] = (x * lax.rsqrt(spread + EPSILON)).astype(jnp.bfloat16)
        up[at : at + cells, :] = fields[at : at + cells, channels:]
    for copy in copies[2 * tiles_count :]:
        copy.wait()

    lane = lax.broadcasted_iota(jnp.int32, (1, LANES), 1)
    low = lane < LANES // 2
    split = 4 * LANES
    extent = WIN
    source = roll_source(codes_ref, lax.broadcasted_iota(jnp.int32, (plane, 1), 0), here, tiles_count, extent)
    from_col = lax.broadcasted_iota(jnp.int32, (plane, plane), 1) == source
    selector = jnp.where(from_col, 1.0, 0.0).astype(jnp.bfloat16)
    source = roll_source(codes_ref, lax.broadcasted_iota(jnp.int32, (1, plane), 1), here, tiles_count, extent)
    from_row = lax.broadcasted_iota(jnp.int32, (plane, plane), 0) == source
    back_selector = jnp.where(from_row, 1.0, 0.0).astype(jnp.bfloat16)
    for l in range(2):
        at = slice(l * plane, (l + 1) * plane)
        front = dot_nn(hid[at, :], wts[:, :split])
        last = dot_nn(hid[at, :], wts[:, split + LANES :])
        back = dot_nn(up[at, :], wts[:, split:])
        mixed = jnp.where(low, last, back[:, LANES:])
        whole = jnp.concatenate([front, back[:, :LANES], mixed], axis=1).astype(jnp.bfloat16)
        rolled[l] = dot_nn(selector, whole).astype(jnp.bfloat16)

    tokens = 2 * cells
    level_k = lax.broadcasted_iota(jnp.int32, (tokens, tokens), 0) // cells
    level_q = lax.broadcasted_iota(jnp.int32, (tokens, tokens), 1) // cells
    allowed = jnp.where((level_k == level_q) | unwrapped, 1.0, 0.0)

    def window(w, carry):
        at = pl.ds(pl.multiple_of(w * cells, cells), cells)
        block = jnp.concatenate([rolled[0, at, :], rolled[1, at, :]], axis=0)
        out = attend_window(block, allowed)
        result[0, at, :] = out[:cells]
        result[1, at, :] = out[cells:]
        return carry

    lax.fori_loop(0, tiles_count, window, 0, unroll=UNROLL)

    zero = jnp.zeros((plane, LANES), jnp.bfloat16)
    for l in range(2):
        at = slice(l * plane, (l + 1) * plane)
        tok = dot_nn(back_selector, result[l]).astype(jnp.bfloat16)
        tail = tok[:, split + LANES :]
        inner_ref[at, :] = jnp.concatenate([tok[:, :split], zero, jnp.where(low, tail, zero)], axis=1)
        outer_ref[at, :] = jnp.concatenate([tok[:, split : split + LANES], jnp.where(low, zero, tail)], axis=1)
    inner, outer = inner_ref[...], outer_ref[...]
    hid_t = hid[...].T
    up_t = up[...].T
    width = 3 * LANES
    share_b = dot_nn(hid_t, inner[:, width:])
    share_b = jnp.concatenate(
        [share_b[:, :LANES], share_b[:, LANES:] + dot_nn(up_t, outer)], axis=1
    ).astype(jnp.bfloat16)
    share_a = dot_nn(hid_t, inner[:, :width]).astype(jnp.bfloat16)
    for share, keep, send in ((share_b, keep_b, send_b), (share_a, keep_a, send_a)):
        for j in range(tiles_count):
            first = share[j * rows : j * rows + half]
            second = share[j * rows + half : (j + 1) * rows]
            keep[j] = jnp.where(rep == 0, first, second)
            send[j] = jnp.where(rep == 0, second, first)


def rows_kernel(inner_any, outer_any, wts_any, keep_ref, send_ref, inner_ref, outer_ref, wts, sems):
    slots, levels, cells, width = keep_ref.shape
    channels = width // 2
    plane = 2 * slots * cells
    split = 4 * LANES
    copies = [
        pltpu.make_async_copy(source, target, sems.at[n])
        for n, (source, target) in enumerate(((inner_any, inner_ref), (outer_any, outer_ref), (wts_any, wts)))
    ]
    for copy in copies:
        copy.start()
    for copy in copies:
        copy.wait()
    for l in range(levels):
        at = slice(l * plane, (l + 1) * plane)
        grad_hidden = dot_nt(inner_ref[at, :], wts[...]).astype(jnp.bfloat16)
        mixed_out = dot_nt(outer_ref[at, :], wts[:, split:]).astype(jnp.bfloat16)
        for k in range(2 * slots):
            ref = send_ref if k % 2 else keep_ref
            at = slice(k * cells, (k + 1) * cells)
            ref[k // 2, l, :, :channels] = mixed_out[at]
            ref[k // 2, l, :, channels:] = grad_hidden[at]


def column_kernel(*refs):
    *slot_refs, out_ref = refs
    here = lax.axis_index("tile")
    blocks = in_order([ref[...] for ref in slot_refs], here)
    pieces = []
    for which in range(2):
        for block in blocks:
            pieces.append(block[:, which * LANES : (which + 1) * LANES])
            rest = 2 * LANES + which * (LANES // 2)
            pieces.append(block[:, rest : rest + LANES // 2])
    out_ref[...] = jnp.concatenate(pieces, axis=1)


SMEM_SPEC = pl.BlockSpec(memory_space=pltpu.SMEM)
VMEM_SPEC = pl.BlockSpec(memory_space=pltpu.VMEM)
ANY_SPEC = pl.BlockSpec(memory_space=pl.ANY)


def call(body, outs, scalars, arrays, flops, mebibytes, scratch=(), spec=VMEM_SPEC):
    moved = sum(a.size * a.dtype.itemsize for a in arrays) + sum(o.size * o.dtype.itemsize for o in outs)
    return pl.pallas_call(
        body,
        out_shape=outs,
        in_specs=[SMEM_SPEC] * len(scalars) + [spec] * len(arrays),
        out_specs=[VMEM_SPEC] * len(outs),
        scratch_shapes=list(scratch),
        compiler_params=pltpu.CompilerParams(vmem_limit_bytes=mebibytes * 1024 * 1024),
        cost_estimate=pl.CostEstimate(flops=flops, bytes_accessed=moved, transcendentals=0),
    )(*scalars, *arrays)


def low_shape(*shape):
    return jax.ShapeDtypeStruct(shape, jnp.bfloat16)


def added(a, b):
    return (a.astype(jnp.float32) + b.astype(jnp.float32)).astype(jnp.bfloat16)


def parted(value, dim, bit):
    size = value.shape[dim] // 2
    keep = lax.dynamic_slice_in_dim(value, bit * size, size, dim)
    send = lax.dynamic_slice_in_dim(value, (1 - bit) * size, size, dim)
    return keep, send


def joined(mine, other, bit, dim=0):
    odd = bit == 1
    return jnp.concatenate([jnp.where(odd, other, mine), jnp.where(odd, mine, other)], axis=dim)


def bits_of(count):
    bits, bit = [], 1
    while bit < count:
        bits.append(bit)
        bit *= 2
    return bits


def reduce_share(keep, send, lev_here, tile_here):
    came = swapped(send, "rep", 1)
    part = added(keep, came)
    for bit in bits_of(lax.axis_size("lev")):
        keep, send = parted(part, 1, (lev_here // bit) % 2)
        came = swapped(send, "lev", bit)
        part = added(keep, came)
    tiles_count = lax.axis_size("tile")
    near = tile_here % 2
    pairs = part.reshape(tiles_count // 2, 2, *part.shape[1:])
    mine = lax.dynamic_index_in_dim(pairs, near, 1, keepdims=False)
    away = lax.dynamic_index_in_dim(pairs, 1 - near, 1, keepdims=False)
    came = swapped(away, "tile", 1)
    both = jnp.stack([mine, came], axis=1)
    far = tile_here // 2
    slots = lax.dynamic_index_in_dim(both, far, 0, keepdims=False)
    found = [slots[0], slots[1]]
    for mask in range(1, tiles_count // 2):
        got = swapped(lax.dynamic_index_in_dim(both, far ^ mask, 0, keepdims=False), "tile", 2 * mask)
        found += [got[0], got[1]]
    rows, cols = part.shape[1:]
    channels = tiles_count * cols // 2
    return call(column_kernel, [low_shape(rows, 2 * channels)], [], found, 1000, 4)[0]


def spread(piece, lev_here):
    for bit in reversed(bits_of(lax.axis_size("lev"))):
        came = swapped(piece, "lev", bit)
        piece = joined(piece, came, (lev_here // bit) % 2)
    came = swapped(piece, "rep", 1)
    return piece, came


def shards_by_heads(tokens, w_qkv, w_proj, seam_codes, upstream):
    levels, extent, channels = tokens.shape[1], tokens.shape[3], tokens.shape[5]
    cells = extent * extent
    tiles_count = lax.axis_size("tile")
    rep_here, lev_here, tile_here = lax.axis_index("rep"), lax.axis_index("lev"), lax.axis_index("tile")
    shard_rows = w_qkv.shape[0]
    field_in = tokens.reshape(levels, cells, channels)
    field_up = upstream.reshape(levels, cells, channels)
    half = shard_rows // 2

    shape = low_shape(cells, 2 * channels)
    high, low, *blocks = call(
        deal_kernel,
        [shape, shape]
        + [low_shape(shard_rows, channels)] * 2
        + [low_shape(half, channels)] * (tiles_count - 2),
        [],
        [w_qkv, w_proj, field_in, field_up],
        1000,
        MAIN_MEBIBYTES,
        scratch=[
            pltpu.VMEM(w_qkv.shape, jnp.bfloat16),
            pltpu.VMEM(w_proj.shape, jnp.bfloat16),
            pltpu.SemaphoreType.DMA((6,)),
        ],
        spec=ANY_SPEC,
    )
    codes, blocks[1] = lax.optimization_barrier((seam_codes.reshape(-1), blocks[1]))
    low = shifted(low, "lev", -1)
    weights = [blocks[0]]
    for k in range(1, tiles_count):
        weights.append(swapped(blocks[k], "tile", k))
        if k >= 2:
            weights.append(swapped(weights[-1], "rep", 1))

    def gathered(piece):
        have = {0: piece}
        for bit in reversed(bits_of(tiles_count)):
            for k in list(have):
                have[k ^ bit] = swapped(have[k], "tile", bit)
        return [have[k] for k in range(tiles_count)]

    pieces = [p for pair in zip(gathered(high), gathered(low)) for p in pair]
    plane = tiles_count * cells
    width = 3 * LANES
    part_shape = low_shape(tiles_count, half, width)
    inner_shape = low_shape(levels * plane, 2 * width)
    outer_shape = low_shape(levels * plane, 2 * LANES)
    weight_shape = low_shape(channels, 2 * width)
    inner, outer, weight, keep_a, send_a, keep_b, send_b = call(
        main_kernel,
        [inner_shape, outer_shape, weight_shape, part_shape, part_shape, part_shape, part_shape],
        [codes],
        [*pieces, *weights],
        8 * levels * plane * channels * channels,
        MAIN_MEBIBYTES,
        scratch=[
            pltpu.VMEM((levels * plane, channels), jnp.bfloat16),
            pltpu.VMEM((levels * plane, channels), jnp.bfloat16),
            pltpu.VMEM((levels, plane, 2 * width), jnp.bfloat16),
            pltpu.VMEM((levels, plane, 2 * width), jnp.bfloat16),
            pltpu.VMEM((levels * plane, 2 * channels), jnp.bfloat16),
            pltpu.SemaphoreType.DMA((len(pieces) + len(weights),)),
        ],
        spec=ANY_SPEC,
    )
    sums_shape = low_shape(tiles_count // 2, levels, cells, 2 * channels)
    keep, send = call(
        rows_kernel,
        [sums_shape, sums_shape],
        [],
        [inner, outer, weight],
        4 * levels * plane * channels * channels // tiles_count,
        MAIN_MEBIBYTES,
        scratch=[
            pltpu.VMEM(inner.shape, jnp.bfloat16),
            pltpu.VMEM(outer.shape, jnp.bfloat16),
            pltpu.VMEM(weight.shape, jnp.bfloat16),
            pltpu.SemaphoreType.DMA((3,)),
        ],
        spec=ANY_SPEC,
    )

    came = swapped(send, "tile", 1)
    sums = added(keep, came)
    slots = [sums[k] for k in range(tiles_count // 2)]
    for bit in bits_of(tiles_count // 2):
        came = swapped(jnp.stack(slots[1::2]), "tile", 2 * bit)
        slots = [added(slots[2 * k], came[k]) for k in range(len(slots) // 2)]
    final = slots[0]
    low_back = shifted(final[1], "lev", 1)
    final = jnp.stack([low_back, final[0]]).reshape(levels * cells, 2 * channels)
    token_rows = field_in.reshape(-1, channels)
    upstream_rows = field_up.reshape(-1, channels)
    normalized, inverse = layer_stats(token_rows)
    output = (token_rows.astype(jnp.float32) + final[:, :channels].astype(jnp.float32)).astype(jnp.bfloat16)
    grad_tokens = norm_backward(upstream_rows, final[:, channels:].astype(jnp.float32), normalized, inverse)

    (own_b, other_b), (own_a, other_a) = [
        spread(reduce_share(*pair, level, tile), level)
        for pair, (level, tile) in (
            ((keep_b, send_b), (lev_here, tile_here)),
            ((keep_a, send_a), lax.optimization_barrier((lev_here, tile_here))),
        )
    ]
    rows = own_a.shape[0]
    grad_qkv = jnp.zeros((shard_rows, 3 * channels), jnp.float32)
    grad_proj = jnp.zeros((shard_rows, channels), jnp.float32)
    for piece_a, piece_b, at in ((own_a, own_b, rep_here * rows), (other_a, other_b, (1 - rep_here) * rows)):
        value, out = piece_b[:, :channels].astype(jnp.float32), piece_b[:, channels:].astype(jnp.float32)
        grad_proj = lax.dynamic_update_slice(grad_proj, out, (at, 0))
        grad_qkv = lax.dynamic_update_slice(grad_qkv, value, (at, 2 * channels))
        grad_qkv = lax.dynamic_update_slice(grad_qkv, piece_a.astype(jnp.float32), (at, 0))
    return (output.reshape(tokens.shape), grad_tokens.reshape(tokens.shape), grad_qkv, grad_proj)


def power_of_two(count):
    return count & (count - 1) == 0


def shards(tokens, w_qkv, w_proj, seam_codes, upstream):
    counts = [lax.axis_size(axis) for axis in ("rep", "lev", "tile")]
    tiles_count = counts[2]
    channels = tokens.shape[5]
    one_window = tokens.shape[0] == 1 and tokens.shape[1] == WIN_LEV and tokens.shape[3] == WIN and tokens.shape[2] == 1
    by_heads = (
        one_window
        and all(power_of_two(count) for count in counts)
        and tiles_count % 4 == 0
        and (channels // HEAD_DIM) % tiles_count == 0
        and channels // tiles_count == LANES + LANES // 2
        and counts[0] == 2
        and (channels // tiles_count) % (8 * counts[0] * counts[1]) == 0
    )
    if not by_heads:
        return shards_general(tokens, w_qkv, w_proj, seam_codes, upstream)
    return shards_by_heads(tokens, w_qkv, w_proj, seam_codes, upstream)


def solution(mesh):
    in_specs = (
        P("rep", "lev", "tile", None, None, None),
        P("tile", None),
        P("tile", None),
        P(),
        P("rep", "lev", "tile", None, None, None),
    )
    out_specs = (
        P("rep", "lev", "tile", None, None, None),
        P("rep", "lev", "tile", None, None, None),
        P("tile", None),
        P("tile", None),
    )
    return jax.shard_map(shards, mesh=mesh, in_specs=in_specs, out_specs=out_specs, check_vma=False)
```

```python
import jax
import jax.numpy as jnp
from jax import lax
from jax.experimental import pallas as pl
from jax.experimental.pallas import tpu as pltpu
from jax.sharding import PartitionSpec as P

HEAD_DIM = 32
WIN = 8
WIN_LEV = 2


EPSILON = 1e-05


def shifted(value, axis, steps):
    count = lax.axis_size(axis)
    pairs = [(source, (source + steps) % count) for source in range(count)]
    return lax.ppermute(value, axis, pairs)


def layer_stats(token_rows):
    values = token_rows.astype(jnp.float32)
    center = jnp.mean(values, axis=1, keepdims=True)
    spread = jnp.mean(jnp.square(values - center), axis=1, keepdims=True)
    inverse = lax.rsqrt(spread + EPSILON)
    return ((values - center) * inverse, inverse)


def norm_backward(upstream_rows, grad_hidden, normalized, inverse):
    centre = jnp.mean(grad_hidden, axis=1, keepdims=True)
    projected = jnp.mean(grad_hidden * normalized, axis=1, keepdims=True)
    total_grad = (
        upstream_rows.astype(jnp.float32)
        + (grad_hidden - centre - normalized * projected) * inverse
    )
    return total_grad.astype(jnp.bfloat16)


def roll_local(grid_field, east_flag, north_flag, north_step):
    shift_cells = WIN // 2
    east_part = shifted(grid_field[:, :, :shift_cells], "tile", -1)
    east_part = jnp.where(east_flag, east_part[:, ::-1], east_part)
    across = jnp.concatenate([grid_field[:, :, shift_cells:], east_part], axis=2)
    north_part = shifted(across[:, :shift_cells], "tile", -north_step)
    north_part = jnp.where(north_flag, north_part[:, :, ::-1], north_part)
    upward = jnp.concatenate([across[:, shift_cells:], north_part], axis=1)
    level_part = shifted(upward[:1], "lev", -1)
    return jnp.concatenate([upward[1:], level_part], axis=0)


def unroll_local(rolled, east_flag, north_flag, north_step):
    shift_cells = WIN // 2
    extent = rolled.shape[1]
    level_part = shifted(rolled[-1:], "lev", 1)
    upward = jnp.concatenate([level_part, rolled[:-1]], axis=0)
    north_part = upward[:, extent - shift_cells :]
    north_part = jnp.where(north_flag, north_part[:, :, ::-1], north_part)
    north_part = shifted(north_part, "tile", north_step)
    across = jnp.concatenate([north_part, upward[:, : extent - shift_cells]], axis=1)
    east_part = across[:, :, extent - shift_cells :]
    east_part = jnp.where(east_flag, east_part[:, ::-1], east_part)
    east_part = shifted(east_part, "tile", 1)
    return jnp.concatenate([east_part, across[:, :, : extent - shift_cells]], axis=2)


def to_windows(grid_field):
    levels = grid_field.shape[0]
    extent = grid_field.shape[1]
    channels = grid_field.shape[3]
    blocks = grid_field.reshape(
        levels // WIN_LEV, WIN_LEV, extent // WIN, WIN, extent // WIN, WIN, channels
    )
    blocks = blocks.transpose(0, 2, 4, 1, 3, 5, 6)
    return blocks.reshape(-1, WIN_LEV * WIN * WIN, channels)


def from_windows(windows, levels, extent):
    channels = windows.shape[-1]
    blocks = windows.reshape(
        levels // WIN_LEV, extent // WIN, extent // WIN, WIN_LEV, WIN, WIN, channels
    )
    blocks = blocks.transpose(0, 3, 1, 4, 2, 5, 6)
    return blocks.reshape(levels, extent, extent, channels)


def split_heads(packed):
    windows = packed.shape[0]
    tokens = packed.shape[1]
    model_width = packed.shape[2] // 3
    head_count = model_width // HEAD_DIM
    query_part = packed[:, :, :model_width].reshape(windows, tokens, head_count, HEAD_DIM)
    key_part = packed[:, :, model_width : 2 * model_width].reshape(
        windows, tokens, head_count, HEAD_DIM
    )
    value_part = packed[:, :, 2 * model_width :].reshape(windows, tokens, head_count, HEAD_DIM)
    return (query_part, key_part, value_part)


def window_mask(wrap_flags, tokens):
    level_of = jnp.arange(tokens, dtype=jnp.int32) // (WIN * WIN)
    same_level = level_of[:, None] == level_of[None, :]
    allowed = jnp.logical_or(
        same_level[None, None], jnp.logical_not(wrap_flags)[:, None, None, None]
    )
    return allowed.astype(jnp.float32)


def attend_forward(packed, wrap_flags):
    query_part, key_part, value_part = split_heads(packed)
    scores = jnp.einsum(
        "wqhd,wkhd->whqk", query_part, key_part, preferred_element_type=jnp.float32
    ) * HEAD_DIM ** (-0.5)
    raised = jnp.exp(scores) * window_mask(wrap_flags, packed.shape[1])
    prob = raised / jnp.sum(raised, axis=-1, keepdims=True)
    prob_low = prob.astype(jnp.bfloat16)
    attended = jnp.einsum(
        "whqk,wkhd->wqhd", prob_low, value_part, preferred_element_type=jnp.float32
    )
    attended = attended.astype(jnp.bfloat16).reshape(packed.shape[0], packed.shape[1], -1)
    return (attended, prob, prob_low)


def attend_backward(packed, back_windows, prob, prob_low):
    query_part, key_part, value_part = split_heads(packed)
    back_heads = back_windows.reshape(query_part.shape)
    grad_value = jnp.einsum(
        "whqk,wqhd->wkhd", prob_low, back_heads, preferred_element_type=jnp.float32
    )
    grad_prob = jnp.einsum(
        "wqhd,wkhd->whqk", back_heads, value_part, preferred_element_type=jnp.float32
    )
    centre = jnp.sum(prob * grad_prob, axis=-1, keepdims=True)
    grad_scores = (prob * (grad_prob - centre) * HEAD_DIM ** (-0.5)).astype(jnp.bfloat16)
    grad_query = jnp.einsum(
        "whqk,wkhd->wqhd", grad_scores, key_part, preferred_element_type=jnp.float32
    )
    grad_key = jnp.einsum(
        "whqk,wqhd->wkhd", grad_scores, query_part, preferred_element_type=jnp.float32
    )
    windows = packed.shape[0]
    tokens = packed.shape[1]
    joined = jnp.concatenate(
        [
            grad_query.reshape(windows, tokens, -1),
            grad_key.reshape(windows, tokens, -1),
            grad_value.reshape(windows, tokens, -1),
        ],
        axis=-1,
    )
    return joined.astype(jnp.bfloat16)


def shards_general(tokens, w_qkv, w_proj, seam_codes, upstream):
    levels = tokens.shape[1]
    extent = tokens.shape[3]
    model_width = tokens.shape[5]
    tiles_count = lax.axis_size("tile")
    north_step = tiles_count // 4
    tile_here = lax.axis_index("tile")
    east_flag = seam_codes[tile_here, 0] == 1
    north_flag = seam_codes[tile_here, 1] == 1
    top_level = lax.axis_index("lev") == lax.axis_size("lev") - 1
    per_level = extent // WIN * (extent // WIN)
    window_total = levels // WIN_LEV * per_level
    lev_window = jnp.arange(window_total, dtype=jnp.int32) // per_level
    wrap_flags = jnp.logical_and(top_level, lev_window == levels // WIN_LEV - 1)
    contract_last = (((1,), (1,)), ((), ()))
    contract_first = (((0,), (0,)), ((), ()))
    grid_in = tokens.reshape(levels, extent, extent, model_width)
    grid_up = upstream.reshape(levels, extent, extent, model_width)
    paired = roll_local(
        jnp.concatenate([grid_in, grid_up], axis=-1), east_flag, north_flag, north_step
    )
    grid_in = paired[..., :model_width]
    grid_up = paired[..., model_width:]
    token_rows = grid_in.reshape(-1, model_width)
    upstream_rows = grid_up.reshape(-1, model_width)
    normalized, inverse = layer_stats(token_rows)
    hidden = normalized.astype(jnp.bfloat16)
    full_qkv, full_proj = (
        lax.all_gather(w_qkv, "tile", axis=0, tiled=True),
        lax.all_gather(w_proj, "tile", axis=0, tiled=True),
    )
    projected = jnp.dot(hidden, full_qkv, preferred_element_type=jnp.float32).astype(jnp.bfloat16)
    grid_qkv = projected.reshape(levels, extent, extent, 3 * model_width)
    windows_qkv = to_windows(grid_qkv)
    attended, prob, prob_low = attend_forward(windows_qkv, wrap_flags)
    grid_mixed = from_windows(attended, levels, extent)
    mixed_in = grid_mixed.reshape(-1, model_width)
    mixed_out = lax.dot_general(
        mixed_in, full_proj, contract_last, preferred_element_type=jnp.float32
    )
    back_mix = jnp.dot(upstream_rows, full_proj, preferred_element_type=jnp.float32)
    output_low = (token_rows.astype(jnp.float32) + mixed_out).astype(jnp.bfloat16)
    back_low = back_mix.astype(jnp.bfloat16)
    grid_back = back_low.reshape(levels, extent, extent, model_width)
    grad_windows = attend_backward(windows_qkv, to_windows(grid_back), prob, prob_low)
    grid_grad = from_windows(grad_windows, levels, extent)
    grad_qkv_tok = grid_grad.reshape(-1, 3 * model_width)
    grad_hidden = lax.dot_general(
        grad_qkv_tok, full_qkv, contract_last, preferred_element_type=jnp.float32
    )
    grad_low = norm_backward(upstream_rows, grad_hidden, normalized, inverse)
    grid_output = output_low.reshape(levels, extent, extent, model_width)
    grid_dx = grad_low.reshape(levels, extent, extent, model_width)
    paired = unroll_local(
        jnp.concatenate([grid_output, grid_dx], axis=-1), east_flag, north_flag, north_step
    )
    grid_output = paired[..., :model_width]
    grid_dx = paired[..., model_width:]
    columns = hidden
    share_qkv = lax.psum_scatter(
        lax.dot_general(
            columns, grad_qkv_tok, contract_first, preferred_element_type=jnp.float32
        ).astype(jnp.bfloat16),
        "tile",
        scatter_dimension=0,
        tiled=True,
    )
    columns = upstream_rows
    share_proj = lax.psum_scatter(
        lax.dot_general(
            columns, mixed_in, contract_first, preferred_element_type=jnp.float32
        ).astype(jnp.bfloat16),
        "tile",
        scatter_dimension=0,
        tiled=True,
    )
    grad_qkv, grad_proj = (
        lax.psum(share_qkv, ("rep", "lev")).astype(jnp.float32),
        lax.psum(share_proj, ("rep", "lev")).astype(jnp.float32),
    )
    return (grid_output.reshape(tokens.shape), grid_dx.reshape(tokens.shape), grad_qkv, grad_proj)


LANES = 128
MAIN_MEBIBYTES = 56
UNROLL = 4
NEAR = LANES // HEAD_DIM


def swapped(value, axis, mask):
    count = lax.axis_size(axis)
    return lax.ppermute(value, axis, [(source, source ^ mask) for source in range(count)])


def roll_source(codes_ref, cell, tile_here, tiles_count, extent):
    half = WIN // 2
    north_step = tiles_count // 4
    slot = cell // (extent * extent)
    row = (cell // extent) % extent
    col = cell % extent

    def code_of(tile, which):
        found = jnp.zeros_like(tile)
        for t in range(tiles_count):
            found = jnp.where(tile == t, codes_ref[2 * t + which], found)
        return found == 1

    tile = jnp.bitwise_xor(slot, tile_here)
    crossed = row >= extent - half
    col1 = jnp.where(crossed & code_of(tile, 1), extent - 1 - col, col)
    row1 = jnp.where(crossed, row - (extent - half), row + half)
    tile1 = jnp.where(crossed, (tile + north_step) % tiles_count, tile)
    crossed = col1 >= extent - half
    row2 = jnp.where(crossed & code_of(tile1, 0), extent - 1 - row1, row1)
    col2 = jnp.where(crossed, col1 - (extent - half), col1 + half)
    tile2 = jnp.where(crossed, (tile1 + 1) % tiles_count, tile1)
    return (jnp.bitwise_xor(tile2, tile_here) * extent + row2) * extent + col2


def in_order(slots, here):
    bit = 1
    while bit < len(slots):
        odd = jnp.bitwise_and(here, bit) != 0
        slots = [jnp.where(odd, slots[k ^ bit], slots[k]) for k in range(len(slots))]
        bit *= 2
    return slots


def dot_nn(a, b):
    return lax.dot_general(a, b, (((1,), (0,)), ((), ())), preferred_element_type=jnp.float32)


def dot_nt(a, b):
    return lax.dot_general(a, b, (((1,), (1,)), ((), ())), preferred_element_type=jnp.float32)


def dot_tn(a, b):
    return lax.dot_general(a, b, (((0,), (0,)), ((), ())), preferred_element_type=jnp.float32)


def deal_kernel(qkv_any, out_any, in_any, up_any, high_ref, low_ref, *refs):
    *block_refs, qkv_ref, out_ref, sems = refs
    tiles_count = len(block_refs)
    channels = out_ref.shape[1]
    own = channels // tiles_count
    rep, here = lax.axis_index("rep"), lax.axis_index("tile")
    copies = [
        pltpu.make_async_copy(source.at[level], target.at[:, first : first + channels], sems.at[2 * level + which])
        for level, target in ((0, low_ref), (1, high_ref))
        for which, (source, first) in enumerate(((in_any, 0), (up_any, channels)))
    ]
    whole = [
        pltpu.make_async_copy(qkv_any, qkv_ref, sems.at[4]),
        pltpu.make_async_copy(out_any, out_ref, sems.at[5]),
    ]
    for copy in [*whole, *copies]:
        copy.start()
    for copy in whole:
        copy.wait()

    def columns(which, tile):
        ref = out_ref if which == 3 else qkv_ref
        base = (0 if which == 3 else which * channels) + tile * own
        return ref[:, base : base + LANES], ref[:, base + LANES : base + own]

    blocks = []
    for tile in range(tiles_count):
        (q, q1), (k, k1), (v, v1), (p, p1) = [columns(which, tile) for which in range(4)]
        blocks.append(jnp.concatenate([q, k, q1, k1, v, p, v1, p1], axis=1))
    for slot, (ref, block) in enumerate(zip(block_refs, in_order(blocks, here))):
        if slot >= 2:
            half = block.shape[0] // 2
            block = jnp.where(rep == 0, block[:half], block[half:])
        ref[...] = block
    for copy in copies:
        copy.wait()


def attend_window(block, allowed):
    tokens = block.shape[0]
    lane = lax.broadcasted_iota(jnp.int32, (1, LANES), 1)
    group = [block[:, g * LANES : (g + 1) * LANES] for g in range(6)]
    scale = HEAD_DIM ** (-0.5)

    def turned(x):
        return pltpu.roll(x.astype(jnp.float32), LANES // 2, 1)

    def attend(q, k, v, o, heads):
        masks = [lane // HEAD_DIM == h for h in range(heads)]

        def stacked(x):
            return jnp.concatenate([jnp.where(m, x, jnp.zeros_like(x)) for m in masks], axis=0)

        def folded(x):
            total = jnp.where(masks[0], x[:tokens], 0.0)
            for h in range(1, heads):
                total = jnp.where(masks[h], x[h * tokens : (h + 1) * tokens], total)
            return total

        k_all, v_all = stacked(k), stacked(v)
        scores = (dot_nt(k_all, q) * scale).reshape(heads, tokens, tokens)
        raised = jnp.exp(scores) * allowed[None]
        prob = raised * (1.0 / jnp.sum(raised, axis=1, keepdims=True))
        grad_prob = dot_nt(v_all, o).reshape(heads, tokens, tokens)
        centre = jnp.sum(prob * grad_prob, axis=1, keepdims=True)
        grad_scores = (prob * (grad_prob - centre) * scale).astype(jnp.bfloat16).reshape(-1, tokens)
        prob_low = prob.astype(jnp.bfloat16).reshape(-1, tokens)
        att = dot_tn(prob_low, v_all)
        grad_q = dot_tn(grad_scores, k_all)
        grad_k = folded(dot_nn(grad_scores, q))
        grad_v = folded(dot_nn(prob_low, o))
        return grad_q, grad_k, grad_v, att

    gq, gk, gv, att = attend(group[0], group[1], group[3], group[4], NEAR)
    qk_turned = turned(group[2]).astype(jnp.bfloat16)
    vo_turned = turned(group[5]).astype(jnp.bfloat16)
    gq1, gk1, gv1, att1 = attend(group[2], qk_turned, group[5], vo_turned, NEAR // 2)
    parts = [gq, gk, gq1 + turned(gk1), gv, att, gv1 + turned(att1)]
    return jnp.concatenate(parts, axis=1).astype(jnp.bfloat16)


def main_kernel(codes_ref, *refs):
    *refs, inner_ref, outer_ref, wts, keep_a, send_a, keep_b, send_b, hid, up, rolled, result, fields, sems = refs
    tiles_count = (len(refs) + 2) // 4
    cells_refs = refs[: 2 * tiles_count]
    near_refs = refs[2 * tiles_count : 2 * tiles_count + 2]
    far_refs = refs[2 * tiles_count + 2 :]
    cells = cells_refs[0].shape[0]
    channels = wts.shape[0]
    rows = channels // tiles_count
    half = rows // 2
    plane = tiles_count * cells
    rep, here = lax.axis_index("rep"), lax.axis_index("tile")
    unwrapped = lax.axis_index("lev") != lax.axis_size("lev") - 1
    copies = []

    def fetch(source, target):
        copy = pltpu.make_async_copy(source, target, sems.at[len(copies)])
        copy.start()
        copies.append(copy)

    for k in range(tiles_count):
        for l in range(2):
            fetch(cells_refs[2 * k + l], fields.at[pl.ds(l * plane + k * cells, cells)])
    for k in range(tiles_count):
        base = (here ^ k) * rows
        if k < 2:
            fetch(near_refs[k], wts.at[pl.ds(pl.multiple_of(base, 32), rows)])
        else:
            fetch(far_refs[2 * k - 4], wts.at[pl.ds(pl.multiple_of(base + rep * half, 32), half)])
            fetch(far_refs[2 * k - 3], wts.at[pl.ds(pl.multiple_of(base + (1 - rep) * half, 32), half)])
    for copy in copies[: 2 * tiles_count]:
        copy.wait()
    for at in range(0, 2 * plane, cells):
        x = fields[at : at + cells, :channels].astype(jnp.float32)
        center = jnp.mean(x, axis=1, keepdims=True)
        x = x - center
        spread = jnp.mean(jnp.square(x), axis=1, keepdims=True)
        hid[at : at + cells, :] = (x * lax.rsqrt(spread + EPSILON)).astype(jnp.bfloat16)
        up[at : at + cells, :] = fields[at : at + cells, channels:]
    for copy in copies[2 * tiles_count :]:
        copy.wait()

    lane = lax.broadcasted_iota(jnp.int32, (1, LANES), 1)
    low = lane < LANES // 2
    split = 4 * LANES
    extent = WIN
    source = roll_source(codes_ref, lax.broadcasted_iota(jnp.int32, (plane, 1), 0), here, tiles_count, extent)
    from_col = lax.broadcasted_iota(jnp.int32, (plane, plane), 1) == source
    selector = jnp.where(from_col, 1.0, 0.0).astype(jnp.bfloat16)
    source = roll_source(codes_ref, lax.broadcasted_iota(jnp.int32, (1, plane), 1), here, tiles_count, extent)
    from_row = lax.broadcasted_iota(jnp.int32, (plane, plane), 0) == source
    back_selector = jnp.where(from_row, 1.0, 0.0).astype(jnp.bfloat16)
    for l in range(2):
        at = slice(l * plane, (l + 1) * plane)
        front = dot_nn(hid[at, :], wts[:, :split])
        last = dot_nn(hid[at, :], wts[:, split + LANES :])
        back = dot_nn(up[at, :], wts[:, split:])
        mixed = jnp.where(low, last, back[:, LANES:])
        whole = jnp.concatenate([front, back[:, :LANES], mixed], axis=1).astype(jnp.bfloat16)
        rolled[l] = dot_nn(selector, whole).astype(jnp.bfloat16)

    tokens = 2 * cells
    level_k = lax.broadcasted_iota(jnp.int32, (tokens, tokens), 0) // cells
    level_q = lax.broadcasted_iota(jnp.int32, (tokens, tokens), 1) // cells
    allowed = jnp.where((level_k == level_q) | unwrapped, 1.0, 0.0)

    def window(w, carry):
        at = pl.ds(pl.multiple_of(w * cells, cells), cells)
        block = jnp.concatenate([rolled[0, at, :], rolled[1, at, :]], axis=0)
        out = attend_window(block, allowed)
        result[0, at, :] = out[:cells]
        result[1, at, :] = out[cells:]
        return carry

    lax.fori_loop(0, tiles_count, window, 0, unroll=UNROLL)

    zero = jnp.zeros((plane, LANES), jnp.bfloat16)
    for l in range(2):
        at = slice(l * plane, (l + 1) * plane)
        tok = dot_nn(back_selector, result[l]).astype(jnp.bfloat16)
        tail = tok[:, split + LANES :]
        inner_ref[at, :] = jnp.concatenate([tok[:, :split], zero, jnp.where(low, tail, zero)], axis=1)
        outer_ref[at, :] = jnp.concatenate([tok[:, split : split + LANES], jnp.where(low, zero, tail)], axis=1)
    inner, outer = inner_ref[...], outer_ref[...]
    hid_t = hid[...].T
    up_t = up[...].T
    width = 3 * LANES
    share_b = dot_nn(hid_t, inner[:, width:])
    share_b = jnp.concatenate(
        [share_b[:, :LANES], share_b[:, LANES:] + dot_nn(up_t, outer)], axis=1
    ).astype(jnp.bfloat16)
    share_a = dot_nn(hid_t, inner[:, :width]).astype(jnp.bfloat16)
    for share, keep, send in ((share_b, keep_b, send_b), (share_a, keep_a, send_a)):
        for j in range(tiles_count):
            first = share[j * rows : j * rows + half]
            second = share[j * rows + half : (j + 1) * rows]
            keep[j] = jnp.where(rep == 0, first, second)
            send[j] = jnp.where(rep == 0, second, first)


def rows_kernel(inner_any, outer_any, wts_any, keep_ref, send_ref, inner_ref, outer_ref, wts, sems):
    slots, levels, cells, width = keep_ref.shape
    channels = width // 2
    plane = 2 * slots * cells
    split = 4 * LANES
    copies = [
        pltpu.make_async_copy(source, target, sems.at[n])
        for n, (source, target) in enumerate(((inner_any, inner_ref), (outer_any, outer_ref), (wts_any, wts)))
    ]
    for copy in copies:
        copy.start()
    for copy in copies:
        copy.wait()
    for l in range(levels):
        at = slice(l * plane, (l + 1) * plane)
        grad_hidden = dot_nt(inner_ref[at, :], wts[...]).astype(jnp.bfloat16)
        mixed_out = dot_nt(outer_ref[at, :], wts[:, split:]).astype(jnp.bfloat16)
        for k in range(2 * slots):
            ref = send_ref if k % 2 else keep_ref
            at = slice(k * cells, (k + 1) * cells)
            ref[k // 2, l, :, :channels] = mixed_out[at]
            ref[k // 2, l, :, channels:] = grad_hidden[at]


def column_kernel(*refs):
    *slot_refs, out_ref = refs
    here = lax.axis_index("tile")
    blocks = in_order([ref[...] for ref in slot_refs], here)
    pieces = []
    for which in range(2):
        for block in blocks:
            pieces.append(block[:, which * LANES : (which + 1) * LANES])
            rest = 2 * LANES + which * (LANES // 2)
            pieces.append(block[:, rest : rest + LANES // 2])
    out_ref[...] = jnp.concatenate(pieces, axis=1)


SMEM_SPEC = pl.BlockSpec(memory_space=pltpu.SMEM)
VMEM_SPEC = pl.BlockSpec(memory_space=pltpu.VMEM)
ANY_SPEC = pl.BlockSpec(memory_space=pl.ANY)


def call(body, outs, scalars, arrays, flops, mebibytes, scratch=(), spec=VMEM_SPEC):
    moved = sum(a.size * a.dtype.itemsize for a in arrays) + sum(o.size * o.dtype.itemsize for o in outs)
    return pl.pallas_call(
        body,
        out_shape=outs,
        in_specs=[SMEM_SPEC] * len(scalars) + [spec] * len(arrays),
        out_specs=[VMEM_SPEC] * len(outs),
        scratch_shapes=list(scratch),
        compiler_params=pltpu.CompilerParams(vmem_limit_bytes=mebibytes * 1024 * 1024),
        cost_estimate=pl.CostEstimate(flops=flops, bytes_accessed=moved, transcendentals=0),
    )(*scalars, *arrays)


def low_shape(*shape):
    return jax.ShapeDtypeStruct(shape, jnp.bfloat16)


def added(a, b):
    return (a.astype(jnp.float32) + b.astype(jnp.float32)).astype(jnp.bfloat16)


def parted(value, dim, bit):
    size = value.shape[dim] // 2
    keep = lax.dynamic_slice_in_dim(value, bit * size, size, dim)
    send = lax.dynamic_slice_in_dim(value, (1 - bit) * size, size, dim)
    return keep, send


def joined(mine, other, bit, dim=0):
    odd = bit == 1
    return jnp.concatenate([jnp.where(odd, other, mine), jnp.where(odd, mine, other)], axis=dim)


def bits_of(count):
    bits, bit = [], 1
    while bit < count:
        bits.append(bit)
        bit *= 2
    return bits


def reduce_share(keep, send, lev_here, tile_here):
    came = swapped(send, "rep", 1)
    part = added(keep, came)
    for bit in bits_of(lax.axis_size("lev")):
        keep, send = parted(part, 1, (lev_here // bit) % 2)
        came = swapped(send, "lev", bit)
        part = added(keep, came)
    tiles_count = lax.axis_size("tile")
    near = tile_here % 2
    pairs = part.reshape(tiles_count // 2, 2, *part.shape[1:])
    mine = lax.dynamic_index_in_dim(pairs, near, 1, keepdims=False)
    away = lax.dynamic_index_in_dim(pairs, 1 - near, 1, keepdims=False)
    came = swapped(away, "tile", 1)
    both = jnp.stack([mine, came], axis=1)
    far = tile_here // 2
    slots = lax.dynamic_index_in_dim(both, far, 0, keepdims=False)
    found = [slots[0], slots[1]]
    for mask in range(1, tiles_count // 2):
        got = swapped(lax.dynamic_index_in_dim(both, far ^ mask, 0, keepdims=False), "tile", 2 * mask)
        found += [got[0], got[1]]
    rows, cols = part.shape[1:]
    channels = tiles_count * cols // 2
    return call(column_kernel, [low_shape(rows, 2 * channels)], [], found, 1000, 4)[0]


def spread(piece, lev_here):
    for bit in reversed(bits_of(lax.axis_size("lev"))):
        came = swapped(piece, "lev", bit)
        piece = joined(piece, came, (lev_here // bit) % 2)
    came = swapped(piece, "rep", 1)
    return piece, came


def shards_by_heads(tokens, w_qkv, w_proj, seam_codes, upstream):
    levels, extent, channels = tokens.shape[1], tokens.shape[3], tokens.shape[5]
    cells = extent * extent
    tiles_count = lax.axis_size("tile")
    rep_here, lev_here, tile_here = lax.axis_index("rep"), lax.axis_index("lev"), lax.axis_index("tile")
    shard_rows = w_qkv.shape[0]
    field_in = tokens.reshape(levels, cells, channels)
    field_up = upstream.reshape(levels, cells, channels)
    half = shard_rows // 2

    shape = low_shape(cells, 2 * channels)
    high, low, *blocks = call(
        deal_kernel,
        [shape, shape]
        + [low_shape(shard_rows, channels)] * 2
        + [low_shape(half, channels)] * (tiles_count - 2),
        [],
        [w_qkv, w_proj, field_in, field_up],
        1000,
        MAIN_MEBIBYTES,
        scratch=[
            pltpu.VMEM(w_qkv.shape, jnp.bfloat16),
            pltpu.VMEM(w_proj.shape, jnp.bfloat16),
            pltpu.SemaphoreType.DMA((6,)),
        ],
        spec=ANY_SPEC,
    )
    codes, blocks[1] = lax.optimization_barrier((seam_codes.reshape(-1), blocks[1]))
    low = shifted(low, "lev", -1)
    weights = [blocks[0]]
    for k in range(1, tiles_count):
        weights.append(swapped(blocks[k], "tile", k))
        if k >= 2:
            weights.append(swapped(weights[-1], "rep", 1))

    def gathered(piece):
        have = {0: piece}
        for bit in reversed(bits_of(tiles_count)):
            for k in list(have):
                have[k ^ bit] = swapped(have[k], "tile", bit)
        return [have[k] for k in range(tiles_count)]

    pieces = [p for pair in zip(gathered(high), gathered(low)) for p in pair]
    plane = tiles_count * cells
    width = 3 * LANES
    part_shape = low_shape(tiles_count, half, width)
    inner_shape = low_shape(levels * plane, 2 * width)
    outer_shape = low_shape(levels * plane, 2 * LANES)
    weight_shape = low_shape(channels, 2 * width)
    inner, outer, weight, keep_a, send_a, keep_b, send_b = call(
        main_kernel,
        [inner_shape, outer_shape, weight_shape, part_shape, part_shape, part_shape, part_shape],
        [codes],
        [*pieces, *weights],
        8 * levels * plane * channels * channels,
        MAIN_MEBIBYTES,
        scratch=[
            pltpu.VMEM((levels * plane, channels), jnp.bfloat16),
            pltpu.VMEM((levels * plane, channels), jnp.bfloat16),
            pltpu.VMEM((levels, plane, 2 * width), jnp.bfloat16),
            pltpu.VMEM((levels, plane, 2 * width), jnp.bfloat16),
            pltpu.VMEM((levels * plane, 2 * channels), jnp.bfloat16),
            pltpu.SemaphoreType.DMA((len(pieces) + len(weights),)),
        ],
        spec=ANY_SPEC,
    )
    sums_shape = low_shape(tiles_count // 2, levels, cells, 2 * channels)
    keep, send = call(
        rows_kernel,
        [sums_shape, sums_shape],
        [],
        [inner, outer, weight],
        4 * levels * plane * channels * channels // tiles_count,
        MAIN_MEBIBYTES,
        scratch=[
            pltpu.VMEM(inner.shape, jnp.bfloat16),
            pltpu.VMEM(outer.shape, jnp.bfloat16),
            pltpu.VMEM(weight.shape, jnp.bfloat16),
            pltpu.SemaphoreType.DMA((3,)),
        ],
        spec=ANY_SPEC,
    )

    came = swapped(send, "tile", 1)
    sums = added(keep, came)
    slots = [sums[k] for k in range(tiles_count // 2)]
    for bit in bits_of(tiles_count // 2):
        came = swapped(jnp.stack(slots[1::2]), "tile", 2 * bit)
        slots = [added(slots[2 * k], came[k]) for k in range(len(slots) // 2)]
    final = slots[0]
    low_back = shifted(final[1], "lev", 1)
    final = jnp.stack([low_back, final[0]]).reshape(levels * cells, 2 * channels)
    token_rows = field_in.reshape(-1, channels)
    upstream_rows = field_up.reshape(-1, channels)
    normalized, inverse = layer_stats(token_rows)
    output = (token_rows.astype(jnp.float32) + final[:, :channels].astype(jnp.float32)).astype(jnp.bfloat16)
    grad_tokens = norm_backward(upstream_rows, final[:, channels:].astype(jnp.float32), normalized, inverse)

    (own_b, other_b), (own_a, other_a) = [
        spread(reduce_share(*pair, level, tile), level)
        for pair, (level, tile) in (
            ((keep_b, send_b), (lev_here, tile_here)),
            ((keep_a, send_a), lax.optimization_barrier((lev_here, tile_here))),
        )
    ]
    rows = own_a.shape[0]
    grad_qkv = jnp.zeros((shard_rows, 3 * channels), jnp.float32)
    grad_proj = jnp.zeros((shard_rows, channels), jnp.float32)
    for piece_a, piece_b, at in ((own_a, own_b, rep_here * rows), (other_a, other_b, (1 - rep_here) * rows)):
        value, out = piece_b[:, :channels].astype(jnp.float32), piece_b[:, channels:].astype(jnp.float32)
        grad_proj = lax.dynamic_update_slice(grad_proj, out, (at, 0))
        grad_qkv = lax.dynamic_update_slice(grad_qkv, value, (at, 2 * channels))
        grad_qkv = lax.dynamic_update_slice(grad_qkv, piece_a.astype(jnp.float32), (at, 0))
    return (output.reshape(tokens.shape), grad_tokens.reshape(tokens.shape), grad_qkv, grad_proj)


def power_of_two(count):
    return count & (count - 1) == 0


def shards(tokens, w_qkv, w_proj, seam_codes, upstream):
    counts = [lax.axis_size(axis) for axis in ("rep", "lev", "tile")]
    tiles_count = counts[2]
    channels = tokens.shape[5]
    one_window = tokens.shape[0] == 1 and tokens.shape[1] == WIN_LEV and tokens.shape[3] == WIN and tokens.shape[2] == 1
    by_heads = (
        one_window
        and all(power_of_two(count) for count in counts)
        and tiles_count % 4 == 0
        and (channels // HEAD_DIM) % tiles_count == 0
        and channels // tiles_count == LANES + LANES // 2
        and counts[0] == 2
        and (channels // tiles_count) % (8 * counts[0] * counts[1]) == 0
    )
    if not by_heads:
        return shards_general(tokens, w_qkv, w_proj, seam_codes, upstream)
    return shards_by_heads(tokens, w_qkv, w_proj, seam_codes, upstream)


def solution(mesh):
    in_specs = (
        P("rep", "lev", "tile", None, None, None),
        P("tile", None),
        P("tile", None),
        P(),
        P("rep", "lev", "tile", None, None, None),
    )
    out_specs = (
        P("rep", "lev", "tile", None, None, None),
        P("rep", "lev", "tile", None, None, None),
        P("tile", None),
        P("tile", None),
    )
    return jax.shard_map(shards, mesh=mesh, in_specs=in_specs, out_specs=out_specs, check_vma=False)
```
